32 devices in a mesh: dp: 4 (over y, z), sp: 8 (over x, core).
Axes of the slice: x: 4, y: 2, z: 2, core: 2. Of those that a mesh axis runs over, the one named last changes fastest.
The devices are a block of a 4x4x8 slice.
Arguments:
- tokens: bfloat16 [32, 16, 64, 1152], P('dp', 'sp'), parts along dimension 0
- caption: bfloat16 [32, 120, 1152], P('dp'), parts along dimension 0
- cap_valid: int32 [32, 120], P('dp'), parts along dimension 0
- time_emb: bfloat16 [32, 6912], P('dp'), parts along dimension 0
- ada_table: bfloat16 [2, 6, 1152], replicated
- attn_wq: bfloat16 [2, 1152, 1152], replicated
- attn_bq: bfloat16 [2, 1152], replicated
- attn_wkv: bfloat16 [2, 1152, 2304], replicated
- attn_bkv: bfloat16 [2, 2304], replicated
- attn_wo: bfloat16 [2, 1152, 1152], replicated
- attn_bo: bfloat16 [2, 1152], replicated
- comp_w: bfloat16 [2, 2, 1152], replicated
- comp_b: bfloat16 [1152], replicated
- cnorm_g: bfloat16 [1152], replicated
- cnorm_b: bfloat16 [1152], replicated
- cross_wq: bfloat16 [2, 1152, 1152], replicated
- cross_bq: bfloat16 [2, 1152], replicated
- cross_wkv: bfloat16 [2, 1152, 2304], replicated
- cross_bkv: bfloat16 [2, 2304], replicated
- cross_wo: bfloat16 [2, 1152, 1152], replicated
- cross_bo: bfloat16 [2, 1152], replicated
- mlp_w1: bfloat16 [2, 1152, 4608], replicated
- mlp_b1: bfloat16 [2, 4608], replicated
- mlp_w2: bfloat16 [2, 4608, 1152], replicated
- mlp_b2: bfloat16 [2, 1152], replicated
Outputs:
- output: bfloat16 [32, 16, 64, 1152], P('dp', 'sp'), parts along dimension 0
There are 4 independent parts. The reference program is written for one: setup_inputs(seed, part) draws one part's arguments, and reference() takes and returns one part's arrays. A program takes and returns all parts, laid end to end along the dimension named above; an argument that names none is the same for every part.
All inputs are finite; a program needn't handle non-finite values.
Results may differ from the reference program's by a relative error of at most 0.0163797.
Values are sent between devices in bfloat16 or wider.
A program may use at most 768 MiB of HBM per device.

```python
import math
import jax
import jax.numpy as jnp
from jax import lax

BATCH_SIZE = 8
GRID_H = 16
GRID_W = 64
MODEL_DIM = 1152
NUM_HEADS = 16
HEAD_DIM = 72
MLP_DIM = 4608
TEXT_LEN = 120

LN_EPS = 1e-6
ATTN_SCALE = HEAD_DIM ** -0.5


def weight_normal(rng_key, arr_shape, fan_in):
    return (jax.random.normal(rng_key, arr_shape, jnp.float32) * fan_in ** -0.5).astype(jnp.bfloat16)


def scaled_normal(rng_key, arr_shape, scale_std, offset):
    return (offset + scale_std * jax.random.normal(rng_key, arr_shape, jnp.float32)).astype(jnp.bfloat16)


def setup_inputs(seed: int = 0, part: int = 0) -> dict:
    part_keys = jax.random.split(jax.random.fold_in(jax.random.key(seed), part), 8)
    shared_keys = jax.random.split(jax.random.key(seed + 1), 21)
    row_pos = jnp.arange(GRID_H, dtype=jnp.float32)[:, None] / GRID_H
    col_pos = jnp.arange(GRID_W, dtype=jnp.float32)[None, :] / GRID_W
    freq_row = jax.random.randint(part_keys[0], (BATCH_SIZE, 4), 1, 4).astype(jnp.float32)
    freq_col = jax.random.randint(part_keys[1], (BATCH_SIZE, 4), 0, 4).astype(jnp.float32)
    mode_phase = jax.random.uniform(part_keys[2], (BATCH_SIZE, 4), jnp.float32, 0.0, 2.0 * math.pi)
    mode_amp = jax.random.normal(part_keys[3], (BATCH_SIZE, 4, MODEL_DIM), jnp.float32)
    mode_angle = 2.0 * math.pi * (freq_row[:, :, None, None] * row_pos + freq_col[:, :, None, None] * col_pos) + mode_phase[:, :, None, None]
    smooth_field = 0.5 * jnp.einsum('bmhw,bmd->bhwd', jnp.cos(mode_angle), mode_amp)
    token_noise = jax.random.normal(part_keys[4], (BATCH_SIZE, GRID_H, GRID_W, MODEL_DIM), jnp.float32)
    cap_len = jax.random.randint(part_keys[6], (BATCH_SIZE, 1), TEXT_LEN // 8, TEXT_LEN + 1)
    return {
        'tokens': (smooth_field + 0.5 * token_noise).astype(jnp.bfloat16),
        'caption': scaled_normal(part_keys[5], (BATCH_SIZE, TEXT_LEN, MODEL_DIM), 1.5, 0.0),
        'cap_valid': (jnp.arange(TEXT_LEN)[None, :] < cap_len).astype(jnp.int32),
        'time_emb': scaled_normal(part_keys[7], (BATCH_SIZE, 6 * MODEL_DIM), 0.7, 0.0),
        'ada_table': scaled_normal(shared_keys[0], (2, 6, MODEL_DIM), 0.7, 0.0),
        'attn_wq': weight_normal(shared_keys[1], (2, MODEL_DIM, MODEL_DIM), MODEL_DIM),
        'attn_bq': scaled_normal(shared_keys[2], (2, MODEL_DIM), 0.5, 0.0),
        'attn_wkv': weight_normal(shared_keys[3], (2, MODEL_DIM, 2 * MODEL_DIM), MODEL_DIM),
        'attn_bkv': scaled_normal(shared_keys[4], (2, 2 * MODEL_DIM), 0.5, 0.0),
        'attn_wo': weight_normal(shared_keys[5], (2, MODEL_DIM, MODEL_DIM), MODEL_DIM),
        'attn_bo': scaled_normal(shared_keys[6], (2, MODEL_DIM), 0.5, 0.0),
        'comp_w': scaled_normal(shared_keys[7], (2, 2, MODEL_DIM), 0.5, 0.0),
        'comp_b': scaled_normal(shared_keys[8], (MODEL_DIM,), 0.5, 0.0),
        'cnorm_g': scaled_normal(shared_keys[9], (MODEL_DIM,), 0.5, 1.0),
        'cnorm_b': scaled_normal(shared_keys[10], (MODEL_DIM,), 0.5, 0.0),
        'cross_wq': weight_normal(shared_keys[11], (2, MODEL_DIM, MODEL_DIM), MODEL_DIM),
        'cross_bq': scaled_normal(shared_keys[12], (2, MODEL_DIM), 0.5, 0.0),
        'cross_wkv': weight_normal(shared_keys[13], (2, MODEL_DIM, 2 * MODEL_DIM), MODEL_DIM),
        'cross_bkv': scaled_normal(shared_keys[14], (2, 2 * MODEL_DIM), 0.5, 0.0),
        'cross_wo': weight_normal(shared_keys[15], (2, MODEL_DIM, MODEL_DIM), MODEL_DIM),
        'cross_bo': scaled_normal(shared_keys[16], (2, MODEL_DIM), 0.5, 0.0),
        'mlp_w1': weight_normal(shared_keys[17], (2, MODEL_DIM, MLP_DIM), MODEL_DIM),
        'mlp_b1': scaled_normal(shared_keys[18], (2, MLP_DIM), 0.5, 0.0),
        'mlp_w2': weight_normal(shared_keys[19], (2, MLP_DIM, MODEL_DIM), MLP_DIM),
        'mlp_b2': scaled_normal(shared_keys[20], (2, MODEL_DIM), 0.5, 0.0),
    }


def layer_norm(values):
    row_mean = jnp.mean(values, axis=-1, keepdims=True)
    centered = values - row_mean
    variance = jnp.mean(centered * centered, axis=-1, keepdims=True)
    return centered * lax.rsqrt(variance + LN_EPS)


def linear(activations, weight, bias_vec):
    flat_acts = activations.reshape(-1, activations.shape[-1])
    result = jnp.dot(flat_acts, weight, preferred_element_type=jnp.float32) + bias_vec.astype(jnp.float32)
    return result.reshape(activations.shape[:-1] + (weight.shape[1],))


def compress(mod_in, conv_w, conv_b, norm_g, norm_b):
    num_batch, num_rows, grid_w, model_dim = mod_in.shape
    grid_view = mod_in.reshape(num_batch, num_rows // 2, 2, grid_w // 2, 2, model_dim).astype(jnp.float32)
    conv_sum = jnp.sum(grid_view * conv_w.astype(jnp.float32)[:, None, :, :], axis=(2, 4)) + conv_b.astype(jnp.float32)
    return (layer_norm(conv_sum) * norm_g.astype(jnp.float32) + norm_b.astype(jnp.float32)).astype(jnp.bfloat16)


def attend(queries, keys_in, values_in, key_bias):
    num_batch, num_query, model_dim = queries.shape
    blk_size = math.gcd(num_query, 128)
    query_blocks = jnp.moveaxis(queries.reshape(num_batch, num_query // blk_size, blk_size, NUM_HEADS, HEAD_DIM), 1, 0).astype(jnp.float32)
    key_heads = keys_in.reshape(num_batch, -1, NUM_HEADS, HEAD_DIM).astype(jnp.float32)
    value_heads = values_in.reshape(num_batch, -1, NUM_HEADS, HEAD_DIM).astype(jnp.float32)

    def one_block(query_blk):
        scores = jnp.einsum('bqhd,bkhd->bhqk', query_blk, key_heads) * ATTN_SCALE
        if key_bias is not None:
            scores = scores + key_bias[:, None, None, :]
        attn_probs = jax.nn.softmax(scores, axis=-1).astype(jnp.bfloat16).astype(jnp.float32)
        return jnp.einsum('bhqk,bkhd->bqhd', attn_probs, value_heads).astype(jnp.bfloat16)

    out_blocks = lax.map(one_block, query_blocks)
    return jnp.moveaxis(out_blocks, 0, 1).reshape(num_batch, num_query, model_dim)


def reference(tokens, caption, cap_valid, time_emb, ada_table, attn_wq, attn_bq, attn_wkv, attn_bkv, attn_wo, attn_bo, comp_w, comp_b, cnorm_g, cnorm_b, cross_wq, cross_bq, cross_wkv, cross_bkv, cross_wo, cross_bo, mlp_w1, mlp_b1, mlp_w2, mlp_b2):
    num_batch = tokens.shape[0]
    model_dim = tokens.shape[3]
    key_bias = jnp.where(cap_valid > 0, 0.0, -1e9).astype(jnp.float32)
    mods_all = time_emb.astype(jnp.float32).reshape(num_batch, 6, model_dim)

    def run_block(hidden, layer_idx):
        mods = (mods_all + ada_table[layer_idx].astype(jnp.float32)[None])[:, :, None, None, :]
        mod_in = (layer_norm(hidden.astype(jnp.float32)) * (1.0 + mods[:, 1]) + mods[:, 0]).astype(jnp.bfloat16)
        queries = linear(mod_in, attn_wq[layer_idx], attn_bq[layer_idx]).astype(jnp.bfloat16).reshape(num_batch, -1, model_dim)
        kv_src = compress(mod_in, comp_w, comp_b, cnorm_g, cnorm_b) if layer_idx == 0 else mod_in
        key_vals = linear(kv_src, attn_wkv[layer_idx], attn_bkv[layer_idx]).astype(jnp.bfloat16).reshape(num_batch, -1, 2 * model_dim)
        attn_out = attend(queries, key_vals[:, :, :model_dim], key_vals[:, :, model_dim:], None)
        attn_proj = linear(attn_out, attn_wo[layer_idx], attn_bo[layer_idx]).reshape(hidden.shape)
        hidden = (hidden.astype(jnp.float32) + mods[:, 2] * attn_proj).astype(jnp.bfloat16)
        cross_q = linear(hidden, cross_wq[layer_idx], cross_bq[layer_idx]).astype(jnp.bfloat16).reshape(num_batch, -1, model_dim)
        cross_kv = linear(caption, cross_wkv[layer_idx], cross_bkv[layer_idx]).astype(jnp.bfloat16)
        cross_out = attend(cross_q, cross_kv[:, :, :model_dim], cross_kv[:, :, model_dim:], key_bias)
        cross_proj = linear(cross_out, cross_wo[layer_idx], cross_bo[layer_idx]).reshape(hidden.shape)
        hidden = (hidden.astype(jnp.float32) + cross_proj).astype(jnp.bfloat16)
        mlp_in = (layer_norm(hidden.astype(jnp.float32)) * (1.0 + mods[:, 4]) + mods[:, 3]).astype(jnp.bfloat16)
        mlp_act = jax.nn.gelu(linear(mlp_in, mlp_w1[layer_idx], mlp_b1[layer_idx]), approximate=True).astype(jnp.bfloat16)
        mlp_out = linear(mlp_act, mlp_w2[layer_idx], mlp_b2[layer_idx])
        return (hidden.astype(jnp.float32) + mods[:, 5] * mlp_out).astype(jnp.bfloat16)

    return run_block(run_block(tokens, 0), 1)
```

```python
import functools, math
import jax, jax.numpy as jnp
from jax import lax
from jax.experimental import pallas as pl
from jax.experimental.pallas import tpu as pltpu
from jax.sharding import PartitionSpec as P

HEAD_DIM = 72
LN_EPS = 1e-6
F32, BF16 = jnp.float32, jnp.bfloat16
SM_SCALE = HEAD_DIM ** -0.5 * math.log2(math.e)
VLIM = 62 * 1024 * 1024


def dotf(a, b):
    return jnp.dot(a, b, preferred_element_type=F32)


def norm(v):
    mean = jnp.mean(v, axis=-1, keepdims=True)
    c = v - mean
    var = jnp.mean(c * c, axis=-1, keepdims=True)
    return c * lax.rsqrt(var + LN_EPS)


def gelu(v):
    k = math.sqrt(2.0 / math.pi)
    t = jnp.tanh(v * (k + (k * 0.044715) * (v * v)))
    hv = 0.5 * v
    return hv + hv * t


def split_heads(ref, val, heads):
    for h in range(heads):
        ref[h] = val[:, h * HEAD_DIM:(h + 1) * HEAD_DIM]


def split_heads_t(ref, val, heads):
    vt = val.T
    for h in range(heads):
        ref[h] = vt[h * HEAD_DIM:(h + 1) * HEAD_DIM, :].astype(BF16)


def attn_head(k, q, vt, bias):
    s = lax.dot_general(k, q, (((1,), (1,)), ((), ())), preferred_element_type=F32)
    if bias is not None:
        s = s + bias
    m = jnp.max(s, axis=0, keepdims=True)
    e = jnp.exp2((s - m) * SM_SCALE)
    l = jnp.sum(e, axis=0, keepdims=True)
    o = dotf(vt, e.astype(BF16))
    return o * (1.0 / l)


def prep0_kernel(x_ref, mods_ref, wq_ref, bq_ref, wkv_ref, bkv_ref, cw_ref, cb_ref, g_ref, b_ref, q_ref, k_ref, v_ref, u_scr, *, layer, width):
    heads = q_ref.shape[0]
    d = x_ref.shape[1]
    u = (norm(x_ref[...].astype(F32)) * (1.0 + mods_ref[1:2, :]) + mods_ref[0:1, :]).astype(BF16)
    q = (dotf(u, wq_ref[...]) + bq_ref[layer:layer + 1, :].astype(F32)).astype(BF16)
    split_heads(q_ref, q, heads)
    uf = u.astype(F32)
    for j in range(d // 128):
        u_scr[j] = uf[:, j * 128:(j + 1) * 128]
    rows = x_ref.shape[0] // width
    parts = []
    for r in range(rows // 2):
        cols = []
        for j in range(d // 128):
            acc = None
            for a in range(2):
                for b in range(2):
                    t = u_scr[j, pl.ds((2 * r + a) * width + b, width // 2, stride=2), :] * cw_ref[a, b:b + 1, j * 128:(j + 1) * 128].astype(F32)
                    acc = t if acc is None else acc + t
            cols.append(acc)
        parts.append(jnp.concatenate(cols, axis=1))
    e = jnp.concatenate(parts, axis=0) + cb_ref[...].astype(F32)
    c = (norm(e) * g_ref[...].astype(F32) + b_ref[...].astype(F32)).astype(BF16)
    kv = dotf(c, wkv_ref[...]) + bkv_ref[layer:layer + 1, :].astype(F32)
    split_heads(k_ref, kv[:, :d].astype(BF16), heads)
    n = kv.shape[0]
    for h in range(heads):
        pass
    vt = kv[:, d:].T
    for h in range(heads):
        v_ref[h] = vt[h * HEAD_DIM:(h + 1) * HEAD_DIM, :].astype(BF16)


def prep1_kernel(x_ref, mods_ref, wq_ref, bq_ref, wkv_ref, bkv_ref, q_ref, k_ref, v_ref, *, layer):
    heads = q_ref.shape[0]
    d = x_ref.shape[1]
    u = (norm(x_ref[...].astype(F32)) * (1.0 + mods_ref[1:2, :]) + mods_ref[0:1, :]).astype(BF16)
    q = (dotf(u, wq_ref[...]) + bq_ref[layer:layer + 1, :].astype(F32)).astype(BF16)
    split_heads(q_ref, q, heads)
    kv = dotf(u, wkv_ref[...]) + bkv_ref[layer:layer + 1, :].astype(F32)
    split_heads(k_ref, kv[:, :d].astype(BF16), heads)
    split_heads_t(v_ref, kv[:, d:], heads)


def full(shape):
    n = len(shape)
    return pl.BlockSpec(shape, lambda *_: (0,) * n, pipeline_mode=pl.Buffered(1))


def layered(shape, layer):
    n = len(shape) - 1
    return pl.BlockSpec((None,) + tuple(shape[1:]), lambda *_: (layer,) + (0,) * n, pipeline_mode=pl.Buffered(1))


def prep(layer, x, mods, wq, bq, wkv, bkv, comp, width):
    t, d = x.shape
    heads = d // HEAD_DIM
    tm = 256
    ins = [x, mods, wq, bq, wkv, bkv]
    specs = [pl.BlockSpec((tm, d), lambda r: (r, 0)), layered(mods.shape, layer), layered(wq.shape, layer), full(bq.shape), layered(wkv.shape, layer), full(bkv.shape)]
    if comp is not None:
        ins += list(comp)
        specs += [full(a.shape) for a in comp]
        nk, kern, scr = tm // 4, functools.partial(prep0_kernel, layer=layer, width=width), [pltpu.VMEM((d // 128, tm, 128), F32)]
    else:
        nk, kern, scr = tm, functools.partial(prep1_kernel, layer=layer), []
    s = t * nk // tm
    if comp is None:
        vshape, vspec = (heads, HEAD_DIM, s), pl.BlockSpec((heads, HEAD_DIM, nk), lambda r: (0, 0, r))
    else:
        vshape, vspec = (t // tm, heads, HEAD_DIM, nk), pl.BlockSpec((None, heads, HEAD_DIM, nk), lambda r: (r, 0, 0, 0))
    q, k, v = pl.pallas_call(
        kern, grid=(t // tm,), in_specs=specs,
        out_specs=[pl.BlockSpec((heads, tm, HEAD_DIM), lambda r: (0, r, 0)), pl.BlockSpec((heads, nk, HEAD_DIM), lambda r: (0, r, 0)), vspec],
        out_shape=[jax.ShapeDtypeStruct((heads, t, HEAD_DIM), BF16), jax.ShapeDtypeStruct((heads, s, HEAD_DIM), BF16), jax.ShapeDtypeStruct(vshape, BF16)],
        scratch_shapes=scr,
        compiler_params=pltpu.CompilerParams(vmem_limit_bytes=VLIM),
        name=f"prep{layer}",
    )(*ins)
    if comp is not None:
        v = jnp.moveaxis(v, 0, 2).reshape(heads, HEAD_DIM, s)
    return q, k, v


def cap_kernel(cap_ref, w_ref, b_ref, k_ref, v_ref, c_scr):
    heads, n, _ = k_ref.shape
    d = cap_ref.shape[1]
    c_scr[...] = jnp.zeros_like(c_scr)
    c_scr[:cap_ref.shape[0], :] = cap_ref[...]
    kv = dotf(c_scr[...], w_ref[...]) + b_ref[...].astype(F32)
    split_heads(k_ref, kv[:, :d].astype(BF16), heads)
    split_heads_t(v_ref, kv[:, d:], heads)


def cap_kv(cap, w, b):
    n, d = cap.shape
    layers = w.shape[0]
    heads = d // HEAD_DIM
    npad = -(-n // 128) * 128
    return pl.pallas_call(
        cap_kernel, grid=(layers,),
        in_specs=[full(cap.shape), pl.BlockSpec((None,) + w.shape[1:], lambda l: (l, 0, 0)), pl.BlockSpec((None, 1, w.shape[2]), lambda l: (l, 0, 0))],
        out_specs=[pl.BlockSpec((None, heads, npad, HEAD_DIM), lambda l: (l, 0, 0, 0)), pl.BlockSpec((None, heads, HEAD_DIM, npad), lambda l: (l, 0, 0, 0))],
        out_shape=[jax.ShapeDtypeStruct((layers, heads, npad, HEAD_DIM), BF16), jax.ShapeDtypeStruct((layers, heads, HEAD_DIM, npad), BF16)],
        scratch_shapes=[pltpu.VMEM((npad, d), BF16)],
        compiler_params=pltpu.CompilerParams(vmem_limit_bytes=VLIM),
        name="capkv",
    )(cap, w, b[:, None, :])


UNROLL = 2


def tail_kernel(x_ref, q_ref, k_ref, v_ref, kc_ref, vc_ref, cb_ref, mods_ref, wo_ref, bo_ref, cwq_ref, cbq_ref, cwo_ref, cbo_ref, w1_ref, b1_ref, w2_ref, b2_ref,
                o_ref, ot_scr, qc_scr, h_scr, *, layer):
    heads = q_ref.shape[0]
    d = x_ref.shape[1]
    f = w1_ref.shape[1]
    row = lambda r: r[layer:layer + 1, :].astype(F32)

    def self_body(h, _):
        ot_scr[h] = attn_head(k_ref[h], q_ref[h], v_ref[h], None)
        return 0

    lax.fori_loop(0, heads, self_body, 0, unroll=UNROLL)
    o = ot_scr[...].reshape(d, -1).T.astype(BF16)
    x = x_ref[...].astype(F32)
    x = (x + mods_ref[2:3, :] * (dotf(o, wo_ref[...]) + row(bo_ref))).astype(BF16)
    qc = (dotf(x, cwq_ref[...]) + row(cbq_ref)).astype(BF16)
    split_heads(qc_scr, qc, heads)
    cbias = cb_ref[...]

    def cross_body(h, _):
        ot_scr[h] = attn_head(kc_ref[h], qc_scr[h], vc_ref[h], cbias)
        return 0

    lax.fori_loop(0, heads, cross_body, 0, unroll=UNROLL)
    o = ot_scr[...].reshape(d, -1).T.astype(BF16)
    x = (x.astype(F32) + (dotf(o, cwo_ref[...]) + row(cbo_ref))).astype(BF16)
    u = (norm(x.astype(F32)) * (1.0 + mods_ref[4:5, :]) + mods_ref[3:4, :]).astype(BF16)
    fb = 512
    for j in range(f // fb):
        sl = slice(j * fb, (j + 1) * fb)
        h_scr[:, sl] = gelu(dotf(u, w1_ref[:, sl]) + b1_ref[layer:layer + 1, sl].astype(F32)).astype(BF16)
    y = dotf(h_scr[...], w2_ref[...]) + row(b2_ref)
    o_ref[...] = (x.astype(F32) + mods_ref[5:6, :] * y).astype(BF16)


def tail(layer, x, q, k, v, kc, vc, cbias, mods, wo, bo, cwq, cbq, cwo, cbo, w1, b1, w2, b2):
    t, d = x.shape
    heads = d // HEAD_DIM
    tm = 256
    L = functools.partial(lambda a: layered(a.shape, layer))
    Fu = lambda a: full(a.shape)
    rowspec = pl.BlockSpec((tm, d), lambda r: (r, 0))
    return pl.pallas_call(
        functools.partial(tail_kernel, layer=layer), grid=(t // tm,),
        in_specs=[rowspec, pl.BlockSpec((heads, tm, HEAD_DIM), lambda r: (0, r, 0)), Fu(k), Fu(v), L(kc), L(vc), Fu(cbias), L(mods), L(wo), Fu(bo), L(cwq), Fu(cbq), L(cwo), Fu(cbo), L(w1), Fu(b1), L(w2), Fu(b2)],
        out_specs=rowspec, out_shape=jax.ShapeDtypeStruct((t, d), BF16),
        scratch_shapes=[pltpu.VMEM((heads, HEAD_DIM, tm), F32), pltpu.VMEM((heads, tm, HEAD_DIM), BF16), pltpu.VMEM((tm, w1.shape[2]), BF16)],
        compiler_params=pltpu.CompilerParams(vmem_limit_bytes=VLIM),
        name=f"tail{layer}",
    )(x, q, k, v, kc, vc, cbias, mods, wo, bo, cwq, cbq, cwo, cbo, w1, b1, w2, b2)


def image_core(x, cap, valid, te, width, ada_table, attn_wq, attn_bq, attn_wkv, attn_bkv, attn_wo, attn_bo, comp_w, comp_b, cnorm_g, cnorm_b, cross_wq, cross_bq, cross_wkv, cross_bkv, cross_wo, cross_bo, mlp_w1, mlp_b1, mlp_w2, mlp_b2):
    d = x.shape[1]
    n = cap.shape[0]
    npad = -(-n // 128) * 128
    mods = te.astype(F32).reshape(6, d)[None] + ada_table.astype(F32)
    cbias = jnp.where(valid > 0, 0.0, -1e9).astype(F32) / HEAD_DIM ** -0.5
    cbias = jnp.pad(cbias, (0, npad - n), constant_values=-jnp.inf)[:, None]
    kc, vc = cap_kv(cap, cross_wkv, cross_bkv)
    comp = (comp_w, comp_b[None], cnorm_g[None], cnorm_b[None])
    for layer in range(2):
        q, k, v = prep(layer, x, mods, attn_wq, attn_bq, attn_wkv, attn_bkv, comp if layer == 0 else None, width)
        x = tail(layer, x, q, k, v, kc, vc, cbias, mods, attn_wo, attn_bo, cross_wq, cross_bq, cross_wo, cross_bo, mlp_w1, mlp_b1, mlp_w2, mlp_b2)
    return x


def exchange_kernel(x_ref, o_ref, send_sem, recv_sem, *, axis):
    n = x_ref.shape[0]
    me = lax.axis_index(axis)
    barrier = pltpu.get_barrier_semaphore()
    for k in range(1, n):
        pl.semaphore_signal(barrier, inc=1, device_id={axis: lax.rem(me + k, n)}, device_id_type=pl.DeviceIdType.MESH)
    pl.semaphore_wait(barrier, n - 1)
    copies = []
    for k in range(1, n):
        peer = lax.rem(me + k, n)
        cp = pltpu.make_async_remote_copy(src_ref=x_ref.at[peer], dst_ref=o_ref.at[me], send_sem=send_sem.at[k - 1], recv_sem=recv_sem.at[k - 1],
                                          device_id={axis: peer}, device_id_type=pl.DeviceIdType.MESH)
        cp.start()
        copies.append(cp)
    o_ref[me] = x_ref[me]
    for cp in copies:
        cp.wait()


def exchange(x, axis, cid):
    n = x.shape[0]
    return pl.pallas_call(
        functools.partial(exchange_kernel, axis=axis),
        in_specs=[pl.BlockSpec(memory_space=pltpu.VMEM)], out_specs=pl.BlockSpec(memory_space=pltpu.VMEM),
        out_shape=jax.ShapeDtypeStruct(x.shape, x.dtype),
        scratch_shapes=[pltpu.SemaphoreType.DMA((n - 1,)), pltpu.SemaphoreType.DMA((n - 1,))],
        compiler_params=pltpu.CompilerParams(collective_id=cid, has_side_effects=True, vmem_limit_bytes=VLIM),
        name=f"exchange{cid}",
    )(x)


def solution(mesh):
    in_specs = (P('dp', 'sp', None, None), P('dp', None, None), P('dp', None), P('dp', None)) + (P(),) * 21
    out_specs = P('dp', 'sp', None, None)
    n = mesh.shape['sp']

    def device_fn(tokens, caption, cap_valid, time_emb, *weights):
        b, rows, width, d = tokens.shape
        assert b == n
        img = lax.axis_index('sp')
        pick = lambda a: lax.dynamic_index_in_dim(a, img, 0, keepdims=False)
        x = exchange(tokens.reshape(b, rows * width, d), 'sp', 0)
        y = image_core(x.reshape(b * rows * width, d), pick(caption), pick(cap_valid), pick(time_emb), width, *weights)
        return exchange(y.reshape(b, rows * width, d), 'sp', 1).reshape(tokens.shape)

    return jax.shard_map(device_fn, mesh=mesh, in_specs=in_specs, out_specs=out_specs, check_vma=False)
```

```python
import functools, math
import jax
import jax.numpy as jnp
from jax import lax
from jax.experimental import pallas as pl
from jax.experimental.pallas import tpu as pltpu
from jax.sharding import PartitionSpec as P

HEAD_DIM = 72
LN_EPS = 1e-6
F32, BF16 = jnp.float32, jnp.bfloat16
SM_SCALE = HEAD_DIM ** -0.5 * math.log2(math.e)
VLIM = 66_900_000
CH = 256
WEIGHTS = ('wq', 'wkv', 'wo', 'cwq', 'cwo', 'w1', 'w2')
SLABS = 4


def dotf(a, b):
    return jnp.dot(a, b, preferred_element_type=F32)


def norm(v):
    mean = jnp.mean(v, axis=-1, keepdims=True)
    c = v - mean
    var = jnp.mean(c * c, axis=-1, keepdims=True)
    return c * lax.rsqrt(var + LN_EPS)


def gelu(v):
    k = math.sqrt(2.0 / math.pi)
    t = jnp.tanh(v * (k + (k * 0.044715) * (v * v)))
    hv = 0.5 * v
    return hv + hv * t


def fold(v, op):
    return op(v.reshape(v.shape[0] // 8, 8, v.shape[1]), axis=0)


def attention(q_at, k_at, v_at, ot_ref, sa, sb, nb, kb_size, heads, bias_at, unroll):
    def scores(h, kb, q):
        s = lax.dot_general(k_at(h, kb), q, (((1,), (1,)), ((), ())), preferred_element_type=F32)
        return s if bias_at is None else s + bias_at(kb)

    def first():
        q = q_at(0)
        mx = None
        for kb in range(nb):
            s = scores(0, kb, q)
            sa[kb * kb_size:(kb + 1) * kb_size, :] = s
            f = fold(s, jnp.max)
            mx = f if mx is None else jnp.maximum(mx, f)
        return mx

    def step(h, hn, mx, cur, nxt):
        m = jnp.max(mx, axis=0, keepdims=True)
        q = q_at(hn)
        mn = l = acc = None
        for kb in range(nb):
            sl = slice(kb * kb_size, (kb + 1) * kb_size)
            s = scores(hn, kb, q)
            nxt[sl, :] = s
            f = fold(s, jnp.max)
            mn = f if mn is None else jnp.maximum(mn, f)
            e = jnp.exp2((cur[sl, :] - m) * SM_SCALE)
            f = fold(e, jnp.sum)
            l = f if l is None else l + f
            a = dotf(v_at(h, kb), e.astype(BF16))
            acc = a if acc is None else acc + a
        l = jnp.sum(l, axis=0, keepdims=True)
        ot_ref[h] = acc * (1.0 / l)
        return mn

    def body(i, mx):
        h = 2 * i
        mx = step(h, h + 1, mx, sa, sb)
        return step(h + 1, jnp.minimum(h + 2, heads - 1), mx, sb, sa)

    lax.fori_loop(0, heads // 2, body, first(), unroll=unroll)


def mega_kernel(*refs, axis, width):
    (x_hbm, cap_hbm, valid_ref, te_ref, tab_ref, bq_ref, bkv_ref, bo_ref, cw_ref, cb_ref, g_ref, gb_ref, cbq_ref, cbkv_ref, cbo_ref, b1_ref, b2_ref,
     wq_hbm, wkv_hbm, wo_hbm, cwq_hbm, cwkv_hbm, cwo_hbm, w1_hbm, w2_hbm, out_hbm,
     wq, wkv, wo, cwq, cwo, w1, w2, x_scr, q_scr, k_scr, vt_scr, kc_scr, vc_scr, cap_scr, vb_scr, bias_scr, mods, sa, sb, sc, sd, ot, h_scr, u_scr, c_scr,
     wsem, csem, xsem, capsem, osem) = refs
    t, d = x_scr.shape
    heads = q_scr.shape[0]
    f = w1.shape[1]
    nkeys0 = t // 4
    ncap = kc_scr.shape[2]
    img = lax.axis_index(axis)
    hbm = dict(zip(WEIGHTS, (wq_hbm, wkv_hbm, wo_hbm, cwq_hbm, cwo_hbm, w1_hbm, w2_hbm)))
    buf = dict(zip(WEIGHTS, (wq, wkv, wo, cwq, cwo, w1, w2)))

    def wcopies(name, layer):
        i = WEIGHTS.index(name)
        rows = buf[name].shape[0] // SLABS
        return [pltpu.make_async_copy(hbm[name].at[layer, pl.ds(s * rows, rows)], buf[name].at[pl.ds(s * rows, rows)], wsem.at[i, s]) for s in range(SLABS)]

    def wstart(name, layer):
        for c in wcopies(name, layer):
            c.start()

    def wwait(name, layer):
        for c in wcopies(name, layer):
            c.wait()

    capcopy = pltpu.make_async_copy(cap_hbm.at[img], cap_scr.at[pl.ds(0, cap_hbm.shape[1])], capsem)
    ccopies = [pltpu.make_async_copy(cwkv_hbm.at[l], w1.at[:, pl.ds(l * 2 * d, 2 * d)], csem.at[l]) for l in range(2)]
    xcopies = [pltpu.make_async_copy(x_hbm.at[pl.ds(c * CH, CH)], x_scr.at[pl.ds(c * CH, CH)], xsem.at[c]) for c in range(t // CH)]
    cap_scr[cap_hbm.shape[1]:, :] = jnp.zeros((ncap - cap_hbm.shape[1], d), BF16)
    capcopy.start()
    for c in ccopies:
        c.start()
    for c in xcopies:
        c.start()
    for name in ('wq', 'wkv', 'wo', 'cwq', 'cwo', 'w2'):
        wstart(name, 0)

    pick = lax.broadcasted_iota(jnp.int32, (te_ref.shape[0], 1), 0) == img
    te = jnp.sum(jnp.where(pick, te_ref[...].astype(F32), 0.0), axis=0, keepdims=True)
    for l in range(2):
        for j in range(6):
            mods[l, j:j + 1, :] = te[:, j * d:(j + 1) * d] + tab_ref[l, j:j + 1, :].astype(F32)
    vb_scr[...] = jnp.full(vb_scr.shape, -jnp.inf, F32)
    valid = jnp.sum(jnp.where(pick, valid_ref[...], 0), axis=0, keepdims=True)
    vb = jnp.where(valid > 0, 0.0, -1e9 / HEAD_DIM ** -0.5).astype(F32)
    vb_scr[:, :valid.shape[1]] = jnp.broadcast_to(vb, (8, valid.shape[1]))
    bias_scr[...] = vb_scr[...].T[:, 0:1]

    def store_heads(ref, rows, val):
        for h in range(heads):
            ref[h, rows, :] = val[:, h * HEAD_DIM:(h + 1) * HEAD_DIM]

    def store_heads_t(ref, cols, val):
        vt = val.T
        for h in range(heads):
            ref[h, :, cols] = vt[h * HEAD_DIM:(h + 1) * HEAD_DIM, :].astype(BF16)

    def row(ref, layer):
        return ref[layer:layer + 1, :].astype(F32)

    def modulate(v, layer, j):
        return (norm(v) * (1.0 + mods[layer, j + 1:j + 2, :]) + mods[layer, j:j + 1, :]).astype(BF16)

    capcopy.wait()
    for l in range(2):
        ccopies[l].wait()
        for part in range(2):
            lo = l * 2 * d + part * d
            y = dotf(cap_scr[...], w1[:, lo:lo + d]) + cbkv_ref[l:l + 1, part * d:(part + 1) * d].astype(F32)
            if part == 0:
                store_heads(kc_scr.at[l], slice(None), y.astype(BF16))
            else:
                store_heads_t(vc_scr.at[l], slice(None), y)
    wstart('w1', 0)

    wwait('wq', 0)
    for c in xcopies:
        c.wait()

    def prep0(c, _):
        rows = pl.ds(pl.multiple_of(c * CH, CH), CH)
        u = modulate(x_scr[rows, :].astype(F32), 0, 0)
        store_heads(q_scr, rows, (dotf(u, wq[...]) + row(bq_ref, 0)).astype(BF16))
        uf = u.astype(F32)
        for j in range(d // 128):
            u_scr[j] = uf[:, j * 128:(j + 1) * 128]
        parts = []
        for r in range(CH // width // 2):
            cols = []
            for j in range(d // 128):
                acc = None
                for a in range(2):
                    for b in range(2):
                        w = cw_ref[a, b:b + 1, j * 128:(j + 1) * 128].astype(F32)
                        v = u_scr[j, pl.ds((2 * r + a) * width + b, width // 2, stride=2), :] * w
                        acc = v if acc is None else acc + v
                cols.append(acc)
            parts.append(jnp.concatenate(cols, axis=1))
        e = jnp.concatenate(parts, axis=0) + cb_ref[...].reshape(1, d).astype(F32)
        y = norm(e) * g_ref[...].reshape(1, d).astype(F32) + gb_ref[...].reshape(1, d).astype(F32)
        c_scr[pl.ds(pl.multiple_of(c * (CH // 4), CH // 4), CH // 4), :] = y.astype(BF16)
        return 0

    lax.fori_loop(0, t // CH, prep0, 0)
    wstart('wq', 1)
    wwait('wkv', 0)
    store_heads(k_scr, slice(0, nkeys0), (dotf(c_scr[...], wkv[:, :d]) + bkv_ref[0:1, :d].astype(F32)).astype(BF16))
    store_heads_t(vt_scr, slice(0, nkeys0), dotf(c_scr[...], wkv[:, d:]) + bkv_ref[0:1, d:].astype(F32))
    wstart('wkv', 1)

    def tail(layer, tq, nkeys, sx, sy, unroll):
        last = t // tq - 1
        kb = min(nkeys, 256)
        halves = tq // CH

        def chunk(c, _):
            base = pl.multiple_of(c * tq, tq)
            rows = pl.ds(base, tq)
            half = [pl.ds(pl.multiple_of(base + i * CH, CH), CH) for i in range(halves)]

            def first_use(name):
                @pl.when(c == 0)
                def _():
                    wwait(name, layer)

            def last_use(name):
                if layer == 0:
                    @pl.when(c == last)
                    def _():
                        wstart(name, 1)

            attention(lambda h: q_scr[h, rows, :], lambda h, i: k_scr[h, i * kb:(i + 1) * kb, :], lambda h, i: vt_scr[h, :, i * kb:(i + 1) * kb],
                      ot.at[:, :, :tq], sx, sy, nkeys // kb, kb, heads, None, unroll)
            first_use('wo')
            first_use('cwq')
            for i in range(halves):
                o = ot[:, :, i * CH:(i + 1) * CH].reshape(d, CH).T.astype(BF16)
                x = x_scr[half[i], :].astype(F32)
                x = (x + mods[layer, 2:3, :] * (dotf(o, wo[...]) + row(bo_ref, layer))).astype(BF16)
                x_scr[half[i], :] = x
                store_heads(q_scr, half[i], (dotf(x, cwq[...]) + row(cbq_ref, layer)).astype(BF16))
            last_use('wo')
            last_use('cwq')
            attention(lambda h: q_scr[h, rows, :], lambda h, i: kc_scr[layer, h], lambda h, i: vc_scr[layer, h],
                      ot.at[:, :, :tq], sc.at[:, :tq], sd.at[:, :tq], 1, ncap, heads, lambda i: bias_scr[...], 8)
            first_use('cwo')
            for i in range(halves):
                o = ot[:, :, i * CH:(i + 1) * CH].reshape(d, CH).T.astype(BF16)
                x_scr[half[i], :] = (x_scr[half[i], :].astype(F32) + (dotf(o, cwo[...]) + row(cbo_ref, layer))).astype(BF16)
            last_use('cwo')
            first_use('w1')
            first_use('w2')

            def mlp(i, _):
                r = pl.ds(pl.multiple_of(base + i * CH, CH), CH)
                u = modulate(x_scr[r, :].astype(F32), layer, 3)
                fb = 512
                for j in range(f // fb):
                    sl = slice(j * fb, (j + 1) * fb)
                    h_scr[:, sl] = gelu(dotf(u, w1[:, sl]) + b1_ref[layer:layer + 1, sl].astype(F32)).astype(BF16)
                y = dotf(h_scr[...], w2[...]) + row(b2_ref, layer)
                x_scr[r, :] = (x_scr[r, :].astype(F32) + mods[layer, 5:6, :] * y).astype(BF16)
                return 0

            if halves == 1:
                mlp(0, 0)
            else:
                lax.fori_loop(0, halves, mlp, 0)
            last_use('w1')
            last_use('w2')
            if layer == 1:
                for i in range(halves):
                    pltpu.make_async_copy(x_scr.at[half[i]], out_hbm.at[half[i]], osem).start()
            return 0

        lax.fori_loop(0, t // tq, chunk, 0)

    tail(0, 2 * CH, nkeys0, sc, sd, 4)

    wwait('wq', 1)
    wwait('wkv', 1)

    def prep1(c, _):
        rows = pl.ds(pl.multiple_of(c * CH, CH), CH)
        u = modulate(x_scr[rows, :].astype(F32), 1, 0)
        store_heads(q_scr, rows, (dotf(u, wq[...]) + row(bq_ref, 1)).astype(BF16))
        store_heads(k_scr, rows, (dotf(u, wkv[:, :d]) + bkv_ref[1:2, :d].astype(F32)).astype(BF16))
        store_heads_t(vt_scr, rows, dotf(u, wkv[:, d:]) + bkv_ref[1:2, d:].astype(F32))
        return 0

    lax.fori_loop(0, t // CH, prep1, 0)
    tail(1, CH, t, sa, sb, 2)
    pltpu.make_async_copy(x_scr, out_hbm, osem).wait()


def image_core(x, caption, cap_valid, time_emb, axis, width, ada_table, attn_wq, attn_bq, attn_wkv, attn_bkv, attn_wo, attn_bo, comp_w, comp_b, cnorm_g, cnorm_b, cross_wq, cross_bq, cross_wkv, cross_bkv, cross_wo, cross_bo, mlp_w1, mlp_b1, mlp_w2, mlp_b2):
    t, d = x.shape
    f = mlp_w1.shape[2]
    heads = d // HEAD_DIM
    ncap = -(-caption.shape[1] // 128) * 128
    vmem = [cap_valid, time_emb, ada_table, attn_bq, attn_bkv, attn_bo, comp_w, comp_b, cnorm_g, cnorm_b, cross_bq, cross_bkv, cross_bo, mlp_b1, mlp_b2]
    weights = [attn_wq, attn_wkv, attn_wo, cross_wq, cross_wkv, cross_wo, mlp_w1, mlp_w2]
    anyspec = pl.BlockSpec(memory_space=pl.ANY)
    V = pltpu.VMEM
    scratch = [V((d, d), BF16), V((d, 2 * d), BF16), V((d, d), BF16), V((d, d), BF16), V((d, d), BF16), V((d, f), BF16), V((f, d), BF16),
               V((t, d), BF16), V((heads, t, HEAD_DIM), BF16), V((heads, t, HEAD_DIM), BF16), V((heads, HEAD_DIM, t), BF16),
               V((2, heads, ncap, HEAD_DIM), BF16), V((2, heads, HEAD_DIM, ncap), BF16), V((ncap, d), BF16), V((8, ncap), F32), V((ncap, 1), F32), V((2, 6, d), F32),
               V((t, CH), F32), V((t, CH), F32), V((t // 4, 2 * CH), F32), V((t // 4, 2 * CH), F32), V((heads, HEAD_DIM, 2 * CH), F32), V((CH, f), BF16),
               V((d // 128, CH, 128), F32), V((t // 4, d), BF16),
               pltpu.SemaphoreType.DMA((len(WEIGHTS), SLABS)), pltpu.SemaphoreType.DMA((2,)), pltpu.SemaphoreType.DMA((t // CH,)), pltpu.SemaphoreType.DMA, pltpu.SemaphoreType.DMA]
    return pl.pallas_call(
        functools.partial(mega_kernel, axis=axis, width=width),
        in_specs=[anyspec, anyspec] + [pl.BlockSpec(memory_space=V)] * len(vmem) + [anyspec] * len(weights),
        out_specs=anyspec, out_shape=jax.ShapeDtypeStruct((t, d), BF16), scratch_shapes=scratch,
        compiler_params=pltpu.CompilerParams(vmem_limit_bytes=VLIM),
        name="blocks",
    )(x, caption, *vmem, *weights)


def exchange_kernel(x_ref, o_ref, send_sem, recv_sem, *, axis):
    n = x_ref.shape[0]
    me = lax.axis_index(axis)
    barrier = pltpu.get_barrier_semaphore()
    for k in range(1, n):
        pl.semaphore_signal(barrier, inc=1, device_id={axis: lax.rem(me + k, n)}, device_id_type=pl.DeviceIdType.MESH)
    pl.semaphore_wait(barrier, n - 1)
    copies = []
    for k in range(1, n):
        peer = lax.rem(me + k, n)
        cp = pltpu.make_async_remote_copy(src_ref=x_ref.at[peer], dst_ref=o_ref.at[me], send_sem=send_sem.at[k - 1], recv_sem=recv_sem.at[k - 1],
                                          device_id={axis: peer}, device_id_type=pl.DeviceIdType.MESH)
        cp.start()
        copies.append(cp)
    o_ref[me] = x_ref[me]
    for cp in copies:
        cp.wait()


def exchange(x, axis, cid):
    n = x.shape[0]
    return pl.pallas_call(
        functools.partial(exchange_kernel, axis=axis),
        in_specs=[pl.BlockSpec(memory_space=pltpu.VMEM)], out_specs=pl.BlockSpec(memory_space=pltpu.VMEM),
        out_shape=jax.ShapeDtypeStruct(x.shape, x.dtype),
        scratch_shapes=[pltpu.SemaphoreType.DMA((n - 1,)), pltpu.SemaphoreType.DMA((n - 1,))],
        compiler_params=pltpu.CompilerParams(collective_id=cid, has_side_effects=True, vmem_limit_bytes=VLIM),
        name=f"exchange{cid}",
    )(x)


def solution(mesh):
    in_specs = (P('dp', 'sp', None, None), P('dp', None, None), P('dp', None), P('dp', None)) + (P(),) * 21
    out_specs = P('dp', 'sp', None, None)
    n = mesh.shape['sp']

    def device_fn(tokens, caption, cap_valid, time_emb, *weights):
        b, rows, width, d = tokens.shape
        assert b == n
        x = exchange(tokens.reshape(b, rows * width, d), 'sp', 0)
        y = image_core(x.reshape(b * rows * width, d), caption, cap_valid, time_emb, 'sp', width, *weights)
        return exchange(y.reshape(b, rows * width, d), 'sp', 1).reshape(tokens.shape)

    return jax.shard_map(device_fn, mesh=mesh, in_specs=in_specs, out_specs=out_specs, check_vma=False)
```

```python
import functools, math
import jax
import jax.numpy as jnp
from jax import lax
from jax.experimental import pallas as pl
from jax.experimental.pallas import tpu as pltpu
from jax.sharding import PartitionSpec as P

HEAD_DIM = 72
LN_EPS = 1e-6
F32, BF16 = jnp.float32, jnp.bfloat16
SM_SCALE = HEAD_DIM ** -0.5 * math.log2(math.e)
VLIM = 66_900_000
CH = 256
WEIGHTS = ('wq', 'wkv', 'wo', 'cwq', 'cwo', 'w1', 'w2')
SLABS = 4


def dotf(a, b):
    return jnp.dot(a, b, preferred_element_type=F32)


def norm(v):
    mean = jnp.mean(v, axis=-1, keepdims=True)
    c = v - mean
    var = jnp.mean(c * c, axis=-1, keepdims=True)
    return c * lax.rsqrt(var + LN_EPS)


def gelu(v):
    k = math.sqrt(2.0 / math.pi)
    t = jnp.tanh(v * (k + (k * 0.044715) * (v * v)))
    hv = 0.5 * v
    return hv + hv * t


def fold(v, op):
    return op(v.reshape(v.shape[0] // 8, 8, v.shape[1]), axis=0)


def attention(q_at, k_at, v_at, ot_ref, sa, sb, nb, kb_size, heads, bias_at, unroll):
    def scores(h, kb, q):
        s = lax.dot_general(k_at(h, kb), q, (((1,), (1,)), ((), ())), preferred_element_type=F32)
        return s if bias_at is None else s + bias_at(kb)

    def first():
        q = q_at(0)
        mx = None
        for kb in range(nb):
            s = scores(0, kb, q)
            sa[kb * kb_size:(kb + 1) * kb_size, :] = s
            f = fold(s, jnp.max)
            mx = f if mx is None else jnp.maximum(mx, f)
        return mx

    def step(h, hn, mx, cur, nxt):
        m = jnp.max(mx, axis=0, keepdims=True)
        q = q_at(hn)
        mn = l = acc = None
        for kb in range(nb):
            sl = slice(kb * kb_size, (kb + 1) * kb_size)
            s = scores(hn, kb, q)
            nxt[sl, :] = s
            f = fold(s, jnp.max)
            mn = f if mn is None else jnp.maximum(mn, f)
            e = jnp.exp2((cur[sl, :] - m) * SM_SCALE)
            f = fold(e, jnp.sum)
            l = f if l is None else l + f
            a = dotf(v_at(h, kb), e.astype(BF16))
            acc = a if acc is None else acc + a
        l = jnp.sum(l, axis=0, keepdims=True)
        ot_ref[h] = acc * (1.0 / l)
        return mn

    def body(i, mx):
        h = 2 * i
        mx = step(h, h + 1, mx, sa, sb)
        return step(h + 1, jnp.minimum(h + 2, heads - 1), mx, sb, sa)

    lax.fori_loop(0, heads // 2, body, first(), unroll=unroll)


def mega_kernel(*refs, axis, width):
    (x_hbm, cap_hbm, valid_ref, te_ref, tab_ref, bq_ref, bkv_ref, bo_ref, cw_ref, cb_ref, g_ref, gb_ref, cbq_ref, cbkv_ref, cbo_ref, b1_ref, b2_ref,
     wq_hbm, wkv_hbm, wo_hbm, cwq_hbm, cwkv_hbm, cwo_hbm, w1_hbm, w2_hbm, out_hbm,
     wq, wkv, wo, cwq, cwo, w1, w2, x_scr, q_scr, k_scr, vt_scr, kc_scr, vc_scr, cap_scr, vb_scr, bias_scr, mods, sa, sb, sc, sd, ot, h_scr, u_scr, c_scr,
     wsem, csem, capsem, in_send, in_recv, out_send, out_recv, own_sem) = refs
    t, d = x_scr.shape
    heads = q_scr.shape[0]
    f = w1.shape[1]
    nkeys0 = t // 4
    ncap = kc_scr.shape[2]
    n, rows_dev = x_hbm.shape[0], x_hbm.shape[1]
    per_chip = CH // rows_dev
    chips = n // per_chip
    img = lax.axis_index(axis)
    my_chip = img // per_chip
    me = img

    def dev_rows(p):
        return pl.ds(pl.multiple_of(p * rows_dev, rows_dev), rows_dev)

    def in_copy(p):
        return pltpu.make_async_remote_copy(src_ref=x_hbm.at[p], dst_ref=x_scr.at[dev_rows(me)], send_sem=in_send.at[p], recv_sem=in_recv.at[me],
                                            device_id={axis: p}, device_id_type=pl.DeviceIdType.MESH)

    def out_copy(p):
        return pltpu.make_async_remote_copy(src_ref=x_scr.at[dev_rows(p)], dst_ref=out_hbm.at[me], send_sem=out_send.at[p], recv_sem=out_recv.at[me],
                                            device_id={axis: p}, device_id_type=pl.DeviceIdType.MESH)

    def ring(k):
        return lax.rem(my_chip + k, chips)

    def in_chip(c):
        return ring(lax.rem(c + c // 2 + 2 * (c // 3), chips))

    def out_chip(c):
        return ring(lax.rem(10 - c + 3 * (c // 2) + 2 * (c // 3), chips))

    barrier = pltpu.get_barrier_semaphore()
    for k in range(1, n):
        pl.semaphore_signal(barrier, inc=1, device_id={axis: lax.rem(me + k, n)}, device_id_type=pl.DeviceIdType.MESH)
    hbm = dict(zip(WEIGHTS, (wq_hbm, wkv_hbm, wo_hbm, cwq_hbm, cwo_hbm, w1_hbm, w2_hbm)))
    buf = dict(zip(WEIGHTS, (wq, wkv, wo, cwq, cwo, w1, w2)))

    def wcopies(name, layer):
        i = WEIGHTS.index(name)
        rows = buf[name].shape[0] // SLABS
        return [pltpu.make_async_copy(hbm[name].at[layer, pl.ds(s * rows, rows)], buf[name].at[pl.ds(s * rows, rows)], wsem.at[i, s]) for s in range(SLABS)]

    def wstart(name, layer):
        for c in wcopies(name, layer):
            c.start()

    def wwait(name, layer):
        for c in wcopies(name, layer):
            c.wait()

    capcopy = pltpu.make_async_copy(cap_hbm.at[img], cap_scr.at[pl.ds(0, cap_hbm.shape[1])], capsem)
    ccopies = [pltpu.make_async_copy(cwkv_hbm.at[l], w1.at[:, pl.ds(l * 2 * d, 2 * d)], csem.at[l]) for l in range(2)]
    own_in = pltpu.make_async_copy(x_hbm.at[me], x_scr.at[dev_rows(me)], own_sem.at[0])
    own_out = pltpu.make_async_copy(x_scr.at[dev_rows(me)], out_hbm.at[me], own_sem.at[1])
    own_in.start()
    partner = me + 1 - 2 * lax.rem(me, per_chip)
    cap_scr[cap_hbm.shape[1]:, :] = jnp.zeros((ncap - cap_hbm.shape[1], d), BF16)
    capcopy.start()
    for c in ccopies:
        c.start()
    pl.semaphore_wait(barrier, n - 1)
    in_copy(partner).start()
    for k in (1, 3, 2):
        for j in range(per_chip):
            in_copy(ring(k) * per_chip + j).start()
    for name in ('wq', 'wkv', 'wo', 'cwq', 'cwo', 'w2'):
        wstart(name, 0)

    pick = lax.broadcasted_iota(jnp.int32, (te_ref.shape[0], 1), 0) == img
    te = jnp.sum(jnp.where(pick, te_ref[...].astype(F32), 0.0), axis=0, keepdims=True)
    for l in range(2):
        for j in range(6):
            mods[l, j:j + 1, :] = te[:, j * d:(j + 1) * d] + tab_ref[l, j:j + 1, :].astype(F32)
    vb_scr[...] = jnp.full(vb_scr.shape, -jnp.inf, F32)
    valid = jnp.sum(jnp.where(pick, valid_ref[...], 0), axis=0, keepdims=True)
    vb = jnp.where(valid > 0, 0.0, -1e9 / HEAD_DIM ** -0.5).astype(F32)
    vb_scr[:, :valid.shape[1]] = jnp.broadcast_to(vb, (8, valid.shape[1]))
    bias_scr[...] = vb_scr[...].T[:, 0:1]

    def store_heads(ref, rows, val):
        for h in range(heads):
            ref[h, rows, :] = val[:, h * HEAD_DIM:(h + 1) * HEAD_DIM]

    def store_heads_t(ref, cols, val):
        vt = val.T
        for h in range(heads):
            ref[h, :, cols] = vt[h * HEAD_DIM:(h + 1) * HEAD_DIM, :].astype(BF16)

    def row(ref, layer):
        return ref[layer:layer + 1, :].astype(F32)

    def modulate(v, layer, j):
        return (norm(v) * (1.0 + mods[layer, j + 1:j + 2, :]) + mods[layer, j:j + 1, :]).astype(BF16)

    capcopy.wait()
    for l in range(2):
        ccopies[l].wait()
        for part in range(2):
            lo = l * 2 * d + part * d
            y = dotf(cap_scr[...], w1[:, lo:lo + d]) + cbkv_ref[l:l + 1, part * d:(part + 1) * d].astype(F32)
            if part == 0:
                store_heads(kc_scr.at[l], slice(None), y.astype(BF16))
            else:
                store_heads_t(vc_scr.at[l], slice(None), y)
    wstart('w1', 0)

    wwait('wq', 0)

    def wait_in(p):
        pltpu.make_async_remote_copy(src_ref=x_hbm.at[p], dst_ref=x_scr.at[dev_rows(p)], send_sem=in_send.at[p], recv_sem=in_recv.at[p],
                                     device_id={axis: p}, device_id_type=pl.DeviceIdType.MESH).wait_recv()

    def prep0(step, _):
        c = in_chip(step)

        @pl.when(step == 0)
        def _():
            own_in.wait()
            wait_in(partner)

        @pl.when(step > 0)
        def _():
            for j in range(per_chip):
                wait_in(c * per_chip + j)

        rows = pl.ds(pl.multiple_of(c * CH, CH), CH)
        u = modulate(x_scr[rows, :].astype(F32), 0, 0)
        store_heads(q_scr, rows, (dotf(u, wq[...]) + row(bq_ref, 0)).astype(BF16))
        uf = u.astype(F32)
        for j in range(d // 128):
            u_scr[j] = uf[:, j * 128:(j + 1) * 128]
        parts = []
        for r in range(CH // width // 2):
            cols = []
            for j in range(d // 128):
                acc = None
                for a in range(2):
                    for b in range(2):
                        w = cw_ref[a, b:b + 1, j * 128:(j + 1) * 128].astype(F32)
                        v = u_scr[j, pl.ds((2 * r + a) * width + b, width // 2, stride=2), :] * w
                        acc = v if acc is None else acc + v
                cols.append(acc)
            parts.append(jnp.concatenate(cols, axis=1))
        e = jnp.concatenate(parts, axis=0) + cb_ref[...].reshape(1, d).astype(F32)
        y = norm(e) * g_ref[...].reshape(1, d).astype(F32) + gb_ref[...].reshape(1, d).astype(F32)
        c_scr[pl.ds(pl.multiple_of(c * (CH // 4), CH // 4), CH // 4), :] = y.astype(BF16)
        return 0

    lax.fori_loop(0, t // CH, prep0, 0)
    wstart('wq', 1)
    in_copy(partner).wait_send()
    for k in (1, 3, 2):
        for j in range(per_chip):
            in_copy(ring(k) * per_chip + j).wait_send()
    wwait('wkv', 0)
    store_heads(k_scr, slice(0, nkeys0), (dotf(c_scr[...], wkv[:, :d]) + bkv_ref[0:1, :d].astype(F32)).astype(BF16))
    store_heads_t(vt_scr, slice(0, nkeys0), dotf(c_scr[...], wkv[:, d:]) + bkv_ref[0:1, d:].astype(F32))
    wstart('wkv', 1)

    def tail(layer, tq, nkeys, sx, sy, unroll):
        last = t // tq - 1
        kb = min(nkeys, 256)
        halves = tq // CH

        def chunk(c, _):
            base = pl.multiple_of((c if layer == 0 else out_chip(c)) * tq, tq)
            rows = pl.ds(base, tq)
            half = [pl.ds(pl.multiple_of(base + i * CH, CH), CH) for i in range(halves)]

            def first_use(name):
                @pl.when(c == 0)
                def _():
                    wwait(name, layer)

            def last_use(name):
                if layer == 0:
                    @pl.when(c == last)
                    def _():
                        wstart(name, 1)

            attention(lambda h: q_scr[h, rows, :], lambda h, i: k_scr[h, i * kb:(i + 1) * kb, :], lambda h, i: vt_scr[h, :, i * kb:(i + 1) * kb],
                      ot.at[:, :, :tq], sx, sy, nkeys // kb, kb, heads, None, unroll)
            first_use('wo')
            first_use('cwq')
            for i in range(halves):
                o = ot[:, :, i * CH:(i + 1) * CH].reshape(d, CH).T.astype(BF16)
                x = x_scr[half[i], :].astype(F32)
                x = (x + mods[layer, 2:3, :] * (dotf(o, wo[...]) + row(bo_ref, layer))).astype(BF16)
                x_scr[half[i], :] = x
                store_heads(q_scr, half[i], (dotf(x, cwq[...]) + row(cbq_ref, layer)).astype(BF16))
            last_use('wo')
            last_use('cwq')
            attention(lambda h: q_scr[h, rows, :], lambda h, i: kc_scr[layer, h], lambda h, i: vc_scr[layer, h],
                      ot.at[:, :, :tq], sc.at[:, :tq], sd.at[:, :tq], 1, ncap, heads, lambda i: bias_scr[...], 8)
            first_use('cwo')
            for i in range(halves):
                o = ot[:, :, i * CH:(i + 1) * CH].reshape(d, CH).T.astype(BF16)
                x_scr[half[i], :] = (x_scr[half[i], :].astype(F32) + (dotf(o, cwo[...]) + row(cbo_ref, layer))).astype(BF16)
            last_use('cwo')
            first_use('w1')
            first_use('w2')

            def mlp(i, _):
                r = pl.ds(pl.multiple_of(base + i * CH, CH), CH)
                u = modulate(x_scr[r, :].astype(F32), layer, 3)
                fb = 512
                for j in range(f // fb):
                    sl = slice(j * fb, (j + 1) * fb)
                    h_scr[:, sl] = gelu(dotf(u, w1[:, sl]) + b1_ref[layer:layer + 1, sl].astype(F32)).astype(BF16)
                y = dotf(h_scr[...], w2[...]) + row(b2_ref, layer)
                x_scr[r, :] = (x_scr[r, :].astype(F32) + mods[layer, 5:6, :] * y).astype(BF16)
                return 0

            if halves == 1:
                mlp(0, 0)
            else:
                lax.fori_loop(0, halves, mlp, 0)
            last_use('w1')
            last_use('w2')
            if layer == 1:
                @pl.when(c < last)
                def _():
                    for j in range(per_chip):
                        out_copy(out_chip(c) * per_chip + j).start()

                @pl.when(c == last)
                def _():
                    out_copy(partner).start()
                    own_out.start()
            return 0

        lax.fori_loop(0, t // tq, chunk, 0)

    tail(0, 2 * CH, nkeys0, sc, sd, 4)

    wwait('wq', 1)
    wwait('wkv', 1)

    def prep1(c, _):
        rows = pl.ds(pl.multiple_of(c * CH, CH), CH)
        u = modulate(x_scr[rows, :].astype(F32), 1, 0)
        store_heads(q_scr, rows, (dotf(u, wq[...]) + row(bq_ref, 1)).astype(BF16))
        store_heads(k_scr, rows, (dotf(u, wkv[:, :d]) + bkv_ref[1:2, :d].astype(F32)).astype(BF16))
        store_heads_t(vt_scr, rows, dotf(u, wkv[:, d:]) + bkv_ref[1:2, d:].astype(F32))
        return 0

    lax.fori_loop(0, t // CH, prep1, 0)
    tail(1, CH, t, sa, sb, 2)

    def wait_out(p):
        pltpu.make_async_remote_copy(src_ref=x_scr.at[dev_rows(p)], dst_ref=out_hbm.at[p], send_sem=out_send.at[p], recv_sem=out_recv.at[p],
                                     device_id={axis: p}, device_id_type=pl.DeviceIdType.MESH).wait_recv()

    own_out.wait()
    for k in range(1, n):
        p = lax.rem(me + k, n)
        out_copy(p).wait_send()
        wait_out(p)


def image_core(x, caption, cap_valid, time_emb, axis, width, ada_table, attn_wq, attn_bq, attn_wkv, attn_bkv, attn_wo, attn_bo, comp_w, comp_b, cnorm_g, cnorm_b, cross_wq, cross_bq, cross_wkv, cross_bkv, cross_wo, cross_bo, mlp_w1, mlp_b1, mlp_w2, mlp_b2):
    n, rows_dev, d = x.shape
    t = n * rows_dev
    f = mlp_w1.shape[2]
    heads = d // HEAD_DIM
    ncap = -(-caption.shape[1] // 128) * 128
    vmem = [cap_valid, time_emb, ada_table, attn_bq, attn_bkv, attn_bo, comp_w, comp_b, cnorm_g, cnorm_b, cross_bq, cross_bkv, cross_bo, mlp_b1, mlp_b2]
    weights = [attn_wq, attn_wkv, attn_wo, cross_wq, cross_wkv, cross_wo, mlp_w1, mlp_w2]
    anyspec = pl.BlockSpec(memory_space=pl.ANY)
    V = pltpu.VMEM
    scratch = [V((d, d), BF16), V((d, 2 * d), BF16), V((d, d), BF16), V((d, d), BF16), V((d, d), BF16), V((d, f), BF16), V((f, d), BF16),
               V((t, d), BF16), V((heads, t, HEAD_DIM), BF16), V((heads, t, HEAD_DIM), BF16), V((heads, HEAD_DIM, t), BF16),
               V((2, heads, ncap, HEAD_DIM), BF16), V((2, heads, HEAD_DIM, ncap), BF16), V((ncap, d), BF16), V((8, ncap), F32), V((ncap, 1), F32), V((2, 6, d), F32),
               V((t, CH), F32), V((t, CH), F32), V((t // 4, 2 * CH), F32), V((t // 4, 2 * CH), F32), V((heads, HEAD_DIM, 2 * CH), F32), V((CH, f), BF16),
               V((d // 128, CH, 128), F32), V((t // 4, d), BF16),
               pltpu.SemaphoreType.DMA((len(WEIGHTS), SLABS)), pltpu.SemaphoreType.DMA((2,)), pltpu.SemaphoreType.DMA] + [pltpu.SemaphoreType.DMA((n,))] * 4 + [pltpu.SemaphoreType.DMA((2,))]
    return pl.pallas_call(
        functools.partial(mega_kernel, axis=axis, width=width),
        in_specs=[anyspec, anyspec] + [pl.BlockSpec(memory_space=V)] * len(vmem) + [anyspec] * len(weights),
        out_specs=anyspec, out_shape=jax.ShapeDtypeStruct(x.shape, BF16), scratch_shapes=scratch,
        compiler_params=pltpu.CompilerParams(collective_id=0, has_side_effects=True, vmem_limit_bytes=VLIM),
        name="blocks",
    )(x, caption, *vmem, *weights)


def solution(mesh):
    in_specs = (P('dp', 'sp', None, None), P('dp', None, None), P('dp', None), P('dp', None)) + (P(),) * 21
    out_specs = P('dp', 'sp', None, None)
    n = mesh.shape['sp']

    def device_fn(tokens, caption, cap_valid, time_emb, *weights):
        b, rows, width, d = tokens.shape
        assert b == n and n * rows * width == 4 * CH and CH % (rows * width) == 0
        return image_core(tokens.reshape(b, rows * width, d), caption, cap_valid, time_emb, 'sp', width, *weights).reshape(tokens.shape)

    return jax.shard_map(device_fn, mesh=mesh, in_specs=in_specs, out_specs=out_specs, check_vma=False)
```

```python
import functools, math
import jax
import jax.numpy as jnp
from jax import lax
from jax.experimental import pallas as pl
from jax.experimental.pallas import tpu as pltpu
from jax.sharding import PartitionSpec as P

HEAD_DIM = 72
LN_EPS = 1e-6
F32, BF16 = jnp.float32, jnp.bfloat16
SM_SCALE = HEAD_DIM ** -0.5 * math.log2(math.e)
VLIM = 64_500_000
CH = 256
WEIGHTS = ('wq', 'wkv', 'wo', 'cwq', 'cwo', 'w1', 'w2')
SLABS = 4


def dotf(a, b):
    return jnp.dot(a, b, preferred_element_type=F32)


def norm(v):
    mean = jnp.mean(v, axis=-1, keepdims=True)
    c = v - mean
    var = jnp.mean(c * c, axis=-1, keepdims=True)
    return c * lax.rsqrt(var + LN_EPS)


def gelu(v):
    k = math.sqrt(2.0 / math.pi)
    t = jnp.tanh(v * (k + (k * 0.044715) * (v * v)))
    hv = 0.5 * v
    return hv + hv * t


def fold(v, op):
    return op(v.reshape(v.shape[0] // 8, 8, v.shape[1]), axis=0)


def attention(q_at, k_at, v_at, ot_ref, sa, sb, nb, kb_size, heads, bias_at, unroll, group=1):
    nkeys = nb * kb_size

    def scores(h, kb, q):
        s = lax.dot_general(k_at(h, kb), q, (((1,), (1,)), ((), ())), preferred_element_type=F32)
        return s if bias_at is None else s + bias_at(kb)

    def form(h, kb, g, q, dst, mx):
        s = scores(h, kb, q)
        dst[g * nkeys + kb * kb_size:g * nkeys + (kb + 1) * kb_size, :] = s
        f = fold(s, jnp.max)
        return f if mx is None else jnp.maximum(mx, f)

    def first():
        out = []
        for g in range(group):
            q = q_at(g)
            mx = None
            for kb in range(nb):
                mx = form(g, kb, g, q, sa, mx)
            out.append(mx)
        return tuple(out)

    def step(i, inext, mxs, cur, nxt):
        out = []
        for g in range(group):
            h, hn = i * group + g, inext * group + g
            m = jnp.max(mxs[g], axis=0, keepdims=True)
            q = q_at(hn)
            mn = l = acc = None
            for kb in range(nb):
                mn = form(hn, kb, g, q, nxt, mn)
                e = jnp.exp2((cur[g * nkeys + kb * kb_size:g * nkeys + (kb + 1) * kb_size, :] - m) * SM_SCALE)
                f = fold(e, jnp.sum)
                l = f if l is None else l + f
                a = dotf(v_at(h, kb), e.astype(BF16))
                acc = a if acc is None else acc + a
            l = jnp.sum(l, axis=0, keepdims=True)
            ot_ref[h] = acc * (1.0 / l)
            out.append(mn)
        return tuple(out)

    def body(j, mxs):
        i = 2 * j
        mxs = step(i, i + 1, mxs, sa, sb)
        return step(i + 1, jnp.minimum(i + 2, heads // group - 1), mxs, sb, sa)

    lax.fori_loop(0, heads // group // 2, body, first(), unroll=unroll)


def mega_kernel(*refs, axis, width):
    (x_hbm, cap_hbm, valid_ref, te_ref, tab_ref, bq_ref, bkv_ref, bo_ref, cw_ref, cb_ref, g_ref, gb_ref, cbq_ref, cbkv_ref, cbo_ref, b1_ref, b2_ref,
     wq_hbm, wkv_hbm, wo_hbm, cwq_hbm, cwkv_hbm, cwo_hbm, w1_hbm, w2_hbm, out_hbm,
     wqkv, wo, cwq, cwo, w1, w2, x_scr, q_scr, k_scr, vt_scr, kc_scr, vc_scr, vb_scr, bias_scr, mods, sa, sb, sc, sd, ot, h_scr, u_scr,
     wsem, csem, capsem, in_send, in_recv, out_send, out_recv, own_sem) = refs
    t, d = x_scr.shape
    heads = q_scr.shape[0]
    f = w1.shape[1]
    nkeys0 = t // 4
    ncap = kc_scr.shape[2]
    n, rows_dev = x_hbm.shape[0], x_hbm.shape[1]
    per_chip = CH // rows_dev
    chips = n // per_chip
    img = lax.axis_index(axis)
    my_chip = img // per_chip
    me = img

    def dev_rows(p):
        return pl.ds(pl.multiple_of(p * rows_dev, rows_dev), rows_dev)

    def in_copy(p):
        return pltpu.make_async_remote_copy(src_ref=x_hbm.at[p], dst_ref=x_scr.at[dev_rows(me)], send_sem=in_send.at[p], recv_sem=in_recv.at[me],
                                            device_id={axis: p}, device_id_type=pl.DeviceIdType.MESH)

    def out_copy(p):
        return pltpu.make_async_remote_copy(src_ref=x_scr.at[dev_rows(p)], dst_ref=out_hbm.at[me], send_sem=out_send.at[p], recv_sem=out_recv.at[me],
                                            device_id={axis: p}, device_id_type=pl.DeviceIdType.MESH)

    def ring(k):
        return lax.rem(my_chip + k, chips)

    def in_chip(c):
        return ring(lax.rem(c + c // 2 + 2 * (c // 3), chips))

    def out_chip(c):
        return ring(lax.rem(10 - c + 3 * (c // 2) + 2 * (c // 3), chips))

    barrier = pltpu.get_barrier_semaphore()
    for k in range(1, n):
        pl.semaphore_signal(barrier, inc=1, device_id={axis: lax.rem(me + k, n)}, device_id_type=pl.DeviceIdType.MESH)
    hbm = dict(zip(WEIGHTS, (wq_hbm, wkv_hbm, wo_hbm, cwq_hbm, cwo_hbm, w1_hbm, w2_hbm)))
    cap_scr, c_scr = h_scr.at[:ncap, 2 * d:3 * d], h_scr.at[:, :d]
    wq, wkv = wqkv.at[:, :d], wqkv.at[:, d:]
    buf = dict(zip(WEIGHTS, (wq, wkv, wo, cwq, cwo, w1, w2)))

    def wcopies(name, layer):
        i = WEIGHTS.index(name)
        rows = buf[name].shape[0] // SLABS
        return [pltpu.make_async_copy(hbm[name].at[layer, pl.ds(s * rows, rows)], buf[name].at[pl.ds(s * rows, rows)], wsem.at[i, s]) for s in range(SLABS)]

    def wstart(name, layer):
        for c in wcopies(name, layer):
            c.start()

    def wwait(name, layer):
        for c in wcopies(name, layer):
            c.wait()

    capcopy = pltpu.make_async_copy(cap_hbm.at[img], cap_scr.at[pl.ds(0, cap_hbm.shape[1])], capsem)
    ccopies = [pltpu.make_async_copy(cwkv_hbm.at[l], w1.at[:, pl.ds(l * 2 * d, 2 * d)], csem.at[l]) for l in range(2)]
    own_in = pltpu.make_async_copy(x_hbm.at[me], x_scr.at[dev_rows(me)], own_sem.at[0])
    own_out = pltpu.make_async_copy(x_scr.at[dev_rows(me)], out_hbm.at[me], own_sem.at[1])
    own_in.start()
    partner = me + 1 - 2 * lax.rem(me, per_chip)
    cap_scr[cap_hbm.shape[1]:, :] = jnp.zeros((ncap - cap_hbm.shape[1], d), BF16)
    capcopy.start()
    for c in ccopies:
        c.start()
    pl.semaphore_wait(barrier, n - 1)
    in_copy(partner).start()
    for k in (1, 3, 2):
        for j in range(per_chip):
            in_copy(ring(k) * per_chip + j).start()
    for name in ('wq', 'wkv', 'wo', 'cwq', 'cwo', 'w2'):
        wstart(name, 0)

    pick = lax.broadcasted_iota(jnp.int32, (te_ref.shape[0], 1), 0) == img
    te = jnp.sum(jnp.where(pick, te_ref[...].astype(F32), 0.0), axis=0, keepdims=True)
    for l in range(2):
        for j in range(6):
            mods[l, j:j + 1, :] = te[:, j * d:(j + 1) * d] + tab_ref[l, j:j + 1, :].astype(F32)
    vb_scr[...] = jnp.full(vb_scr.shape, -jnp.inf, F32)
    valid = jnp.sum(jnp.where(pick, valid_ref[...], 0), axis=0, keepdims=True)
    vb = jnp.where(valid > 0, 0.0, -1e9 / HEAD_DIM ** -0.5).astype(F32)
    vb_scr[:, :valid.shape[1]] = jnp.broadcast_to(vb, (8, valid.shape[1]))
    bias_scr[...] = vb_scr[...].T[:, 0:1]

    def store_heads(ref, rows, val):
        for h in range(heads):
            ref[h, rows, :] = val[:, h * HEAD_DIM:(h + 1) * HEAD_DIM]

    def store_heads_t(ref, cols, val):
        vt = val.T
        for h in range(heads):
            ref[h, :, cols] = vt[h * HEAD_DIM:(h + 1) * HEAD_DIM, :].astype(BF16)

    def row(ref, layer):
        return ref[layer:layer + 1, :].astype(F32)

    def modulate(v, layer, j):
        return (norm(v) * (1.0 + mods[layer, j + 1:j + 2, :]) + mods[layer, j:j + 1, :]).astype(BF16)

    capcopy.wait()
    for l in range(2):
        ccopies[l].wait()
        for part in range(2):
            lo = l * 2 * d + part * d
            y = dotf(cap_scr[...], w1[:, lo:lo + d]) + cbkv_ref[l:l + 1, part * d:(part + 1) * d].astype(F32)
            if part == 0:
                store_heads(kc_scr.at[l], slice(None), y.astype(BF16))
            else:
                store_heads_t(vc_scr.at[l], slice(None), y)
    wstart('w1', 0)

    wwait('wq', 0)

    def wait_in(p):
        pltpu.make_async_remote_copy(src_ref=x_hbm.at[p], dst_ref=x_scr.at[dev_rows(p)], send_sem=in_send.at[p], recv_sem=in_recv.at[p],
                                     device_id={axis: p}, device_id_type=pl.DeviceIdType.MESH).wait_recv()

    def prep0(step, _):
        c = in_chip(step)

        @pl.when(step == 0)
        def _():
            own_in.wait()
            wait_in(partner)

        @pl.when(step > 0)
        def _():
            for j in range(per_chip):
                wait_in(c * per_chip + j)

        rows = pl.ds(pl.multiple_of(c * CH, CH), CH)
        u = modulate(x_scr[rows, :].astype(F32), 0, 0)
        store_heads(q_scr, rows, (dotf(u, wq[...]) + row(bq_ref, 0)).astype(BF16))
        uf = u.astype(F32)
        parts = []
        for r in range(CH // width // 2):
            cols = []
            for j in range(d // 128):
                u_scr[j] = uf[2 * r * width:2 * (r + 1) * width, j * 128:(j + 1) * 128]
                acc = None
                for a in range(2):
                    for b in range(2):
                        w = cw_ref[a, b:b + 1, j * 128:(j + 1) * 128].astype(F32)
                        v = u_scr[j, pl.ds(a * width + b, width // 2, stride=2), :] * w
                        acc = v if acc is None else acc + v
                cols.append(acc)
            parts.append(jnp.concatenate(cols, axis=1))
        e = jnp.concatenate(parts, axis=0) + cb_ref[...].reshape(1, d).astype(F32)
        y = norm(e) * g_ref[...].reshape(1, d).astype(F32) + gb_ref[...].reshape(1, d).astype(F32)
        c_scr[pl.ds(pl.multiple_of(c * (CH // 4), CH // 4), CH // 4), :] = y.astype(BF16)
        return 0

    lax.fori_loop(0, t // CH, prep0, 0)
    wstart('wq', 1)
    in_copy(partner).wait_send()
    for k in (1, 3, 2):
        for j in range(per_chip):
            in_copy(ring(k) * per_chip + j).wait_send()
    wwait('wkv', 0)
    y = dotf(c_scr[...], wkv[...]) + row(bkv_ref, 0)
    store_heads(k_scr, slice(0, nkeys0), y[:, :d].astype(BF16))
    store_heads_t(vt_scr, slice(0, nkeys0), y[:, d:])
    wstart('wkv', 1)

    def tail(layer, tq, nkeys, sx, sy, unroll, cg):
        for name in ('wo', 'cwq', 'cwo', 'w1', 'w2'):
            wwait(name, layer)
        last = t // tq - 1
        kb = min(nkeys, 256)
        halves = tq // CH

        def chunk(c, _):
            base = pl.multiple_of((c if layer == 0 else out_chip(c)) * tq, tq)
            rows = pl.ds(base, tq)
            half = [pl.ds(pl.multiple_of(base + i * CH, CH), CH) for i in range(halves)]

            attention(lambda h: q_scr[h, rows, :], lambda h, i: k_scr[h, i * kb:(i + 1) * kb, :], lambda h, i: vt_scr[h, :, i * kb:(i + 1) * kb],
                      ot.at[:, :, :tq], sx, sy, nkeys // kb, kb, heads, None, unroll)
            for i in range(halves):
                o = ot[:, :, i * CH:(i + 1) * CH].reshape(d, CH).T.astype(BF16)
                x = x_scr[half[i], :].astype(F32)
                x = (x + mods[layer, 2:3, :] * (dotf(o, wo[...]) + row(bo_ref, layer))).astype(BF16)
                x_scr[half[i], :] = x
                store_heads(q_scr, half[i], (dotf(x, cwq[...]) + row(cbq_ref, layer)).astype(BF16))
            attention(lambda h: q_scr[h, rows, :], lambda h, i: kc_scr[layer, h], lambda h, i: vc_scr[layer, h],
                      ot.at[:, :, :tq], sx, sy, 1, ncap, heads, lambda i: bias_scr[...], heads // cg // 2, cg)
            for i in range(halves):
                o = ot[:, :, i * CH:(i + 1) * CH].reshape(d, CH).T.astype(BF16)
                x_scr[half[i], :] = (x_scr[half[i], :].astype(F32) + (dotf(o, cwo[...]) + row(cbo_ref, layer))).astype(BF16)

            def mlp(i, _):
                r = pl.ds(pl.multiple_of(base + i * CH, CH), CH)
                u = modulate(x_scr[r, :].astype(F32), layer, 3)
                fb = 512
                for j in range(f // fb):
                    sl = slice(j * fb, (j + 1) * fb)
                    h_scr[:, sl] = gelu(dotf(u, w1[:, sl]) + b1_ref[layer:layer + 1, sl].astype(F32)).astype(BF16)
                y = dotf(h_scr[...], w2[...]) + row(b2_ref, layer)
                x_scr[r, :] = (x_scr[r, :].astype(F32) + mods[layer, 5:6, :] * y).astype(BF16)
                return 0

            if halves == 1:
                mlp(0, 0)
            else:
                lax.fori_loop(0, halves, mlp, 0)
            if layer == 1:
                @pl.when(c < last)
                def _():
                    for j in range(per_chip):
                        out_copy(out_chip(c) * per_chip + j).start()

                @pl.when(c == last)
                def _():
                    out_copy(partner).start()
                    own_out.start()
            return 0

        lax.fori_loop(0, t // tq, chunk, 0)

    tail(0, 2 * CH, nkeys0, sc, sd, 4, 2)
    for name in ('wo', 'cwq', 'cwo', 'w1', 'w2'):
        wstart(name, 1)

    wwait('wq', 1)
    wwait('wkv', 1)

    def prep1(c, _):
        rows = pl.ds(pl.multiple_of(c * CH, CH), CH)
        u = modulate(x_scr[rows, :].astype(F32), 1, 0)
        y = dotf(u, wqkv[...])
        store_heads(q_scr, rows, (y[:, :d] + row(bq_ref, 1)).astype(BF16))
        store_heads(k_scr, rows, (y[:, d:2 * d] + bkv_ref[1:2, :d].astype(F32)).astype(BF16))
        store_heads_t(vt_scr, rows, y[:, 2 * d:] + bkv_ref[1:2, d:].astype(F32))
        return 0

    lax.fori_loop(0, t // CH, prep1, 0)
    tail(1, CH, t, sa, sb, 4, 4)

    def wait_out(p):
        pltpu.make_async_remote_copy(src_ref=x_scr.at[dev_rows(p)], dst_ref=out_hbm.at[p], send_sem=out_send.at[p], recv_sem=out_recv.at[p],
                                     device_id={axis: p}, device_id_type=pl.DeviceIdType.MESH).wait_recv()

    own_out.wait()
    for k in range(1, n):
        p = lax.rem(me + k, n)
        out_copy(p).wait_send()
        wait_out(p)


def image_core(x, caption, cap_valid, time_emb, axis, width, ada_table, attn_wq, attn_bq, attn_wkv, attn_bkv, attn_wo, attn_bo, comp_w, comp_b, cnorm_g, cnorm_b, cross_wq, cross_bq, cross_wkv, cross_bkv, cross_wo, cross_bo, mlp_w1, mlp_b1, mlp_w2, mlp_b2):
    n, rows_dev, d = x.shape
    t = n * rows_dev
    f = mlp_w1.shape[2]
    heads = d // HEAD_DIM
    ncap = -(-caption.shape[1] // 128) * 128
    vmem = [cap_valid, time_emb, ada_table, attn_bq, attn_bkv, attn_bo, comp_w, comp_b, cnorm_g, cnorm_b, cross_bq, cross_bkv, cross_bo, mlp_b1, mlp_b2]
    weights = [attn_wq, attn_wkv, attn_wo, cross_wq, cross_wkv, cross_wo, mlp_w1, mlp_w2]
    anyspec = pl.BlockSpec(memory_space=pl.ANY)
    V = pltpu.VMEM
    scratch = [V((d, 3 * d), BF16), V((d, d), BF16), V((d, d), BF16), V((d, d), BF16), V((d, f), BF16), V((f, d), BF16),
               V((t, d), BF16), V((heads, t, HEAD_DIM), BF16), V((heads, t, HEAD_DIM), BF16), V((heads, HEAD_DIM, t), BF16),
               V((2, heads, ncap, HEAD_DIM), BF16), V((2, heads, HEAD_DIM, ncap), BF16), V((8, ncap), F32), V((ncap, 1), F32), V((2, 6, d), F32),
               V((t, CH), F32), V((t, CH), F32), V((t // 4, 2 * CH), F32), V((t // 4, 2 * CH), F32), V((heads, HEAD_DIM, 2 * CH), F32), V((CH, f), BF16),
               V((d // 128, 2 * width, 128), F32),
               pltpu.SemaphoreType.DMA((len(WEIGHTS), SLABS)), pltpu.SemaphoreType.DMA((2,)), pltpu.SemaphoreType.DMA] + [pltpu.SemaphoreType.DMA((n,))] * 4 + [pltpu.SemaphoreType.DMA((2,))]
    return pl.pallas_call(
        functools.partial(mega_kernel, axis=axis, width=width),
        in_specs=[anyspec, anyspec] + [pl.BlockSpec(memory_space=V)] * len(vmem) + [anyspec] * len(weights),
        out_specs=pl.BlockSpec(memory_space=V), out_shape=V(x.shape, BF16), scratch_shapes=scratch,
        compiler_params=pltpu.CompilerParams(collective_id=0, has_side_effects=True, vmem_limit_bytes=VLIM),
        name="blocks",
    )(x, caption, *vmem, *weights)


def solution(mesh):
    in_specs = (P('dp', 'sp', None, None), P('dp', None, None), P('dp', None), P('dp', None)) + (P(),) * 21
    out_specs = P('dp', 'sp', None, None)
    n = mesh.shape['sp']

    def device_fn(tokens, caption, cap_valid, time_emb, *weights):
        b, rows, width, d = tokens.shape
        assert b == n and n * rows * width == 4 * CH and CH % (rows * width) == 0
        return image_core(tokens.reshape(b, rows * width, d), caption, cap_valid, time_emb, 'sp', width, *weights).reshape(tokens.shape)

    return jax.shard_map(device_fn, mesh=mesh, in_specs=in_specs, out_specs=out_specs, check_vma=False)
```

```python
import functools, math
import jax
import jax.numpy as jnp
from jax import lax
from jax.experimental import pallas as pl
from jax.experimental.pallas import tpu as pltpu
from jax.sharding import PartitionSpec as P

HEAD_DIM = 72
LN_EPS = 1e-6
F32, BF16 = jnp.float32, jnp.bfloat16
SM_SCALE = HEAD_DIM ** -0.5 * math.log2(math.e)
VLIM = 64_500_000
CH = 256
WEIGHTS = ('wq', 'wkv', 'wo', 'cwq', 'cwo', 'w1', 'w2')
SLABS = 4


def dotf(a, b):
    return jnp.dot(a, b, preferred_element_type=F32)


def norm(v):
    mean = jnp.mean(v, axis=-1, keepdims=True)
    c = v - mean
    var = jnp.mean(c * c, axis=-1, keepdims=True)
    return c * lax.rsqrt(var + LN_EPS)


def gelu(v):
    k = math.sqrt(2.0 / math.pi)
    t = jnp.tanh(v * (k + (k * 0.044715) * (v * v)))
    hv = 0.5 * v
    return hv + hv * t


def fold(v, op):
    return op(v.reshape(v.shape[0] // 8, 8, v.shape[1]), axis=0)


def attention(q_at, k_at, v_at, ot_ref, sa, sb, nb, kb_size, heads, bias_at, unroll, group=1):
    nkeys = nb * kb_size

    def scores(h, kb, q):
        s = lax.dot_general(k_at(h, kb), q, (((1,), (1,)), ((), ())), preferred_element_type=F32)
        return s if bias_at is None else s + bias_at(kb)

    def form(h, kb, g, q, dst, mx):
        s = scores(h, kb, q)
        dst[g * nkeys + kb * kb_size:g * nkeys + (kb + 1) * kb_size, :] = s
        f = fold(s, jnp.max)
        return f if mx is None else jnp.maximum(mx, f)

    def first():
        out = []
        for g in range(group):
            q = q_at(g)
            mx = None
            for kb in range(nb):
                mx = form(g, kb, g, q, sa, mx)
            out.append(mx)
        return tuple(out)

    def step(i, inext, mxs, cur, nxt):
        out = []
        for g in range(group):
            h, hn = i * group + g, inext * group + g
            m = jnp.max(mxs[g], axis=0, keepdims=True)
            q = q_at(hn)
            mn = l = acc = None
            for kb in range(nb):
                mn = form(hn, kb, g, q, nxt, mn)
                e = jnp.exp2((cur[g * nkeys + kb * kb_size:g * nkeys + (kb + 1) * kb_size, :] - m) * SM_SCALE)
                f = fold(e, jnp.sum)
                l = f if l is None else l + f
                a = dotf(v_at(h, kb), e.astype(BF16))
                acc = a if acc is None else acc + a
            l = jnp.sum(l, axis=0, keepdims=True)
            ot_ref[h] = acc * (1.0 / l)
            out.append(mn)
        return tuple(out)

    def body(j, mxs):
        i = 2 * j
        mxs = step(i, i + 1, mxs, sa, sb)
        return step(i + 1, jnp.minimum(i + 2, heads // group - 1), mxs, sb, sa)

    lax.fori_loop(0, heads // group // 2, body, first(), unroll=unroll)


def mega_kernel(*refs, axis, width):
    (x_hbm, cap_hbm, valid_ref, te_ref, tab_ref, bq_ref, bkv_ref, bo_ref, cw_ref, cb_ref, g_ref, gb_ref, cbq_ref, cbkv_ref, cbo_ref, b1_ref, b2_ref,
     wq_hbm, wkv_hbm, wo_hbm, cwq_hbm, cwkv_hbm, cwo_hbm, w1_hbm, w2_hbm, out_hbm,
     wqkv, wo, cwq, cwo, w1, w2, x_scr, q_scr, k_scr, vt_scr, kc_scr, vc_scr, vb_scr, bias_scr, mods, sa, sb, sc, sd, ot, h_scr, u_scr,
     wsem, csem, capsem, in_send, in_recv, out_send, out_recv, own_sem) = refs
    t, d = x_scr.shape
    heads = q_scr.shape[0]
    f = w1.shape[1]
    nkeys0 = t // 4
    ncap = kc_scr.shape[2]
    n, rows_dev = x_hbm.shape[0], x_hbm.shape[1]
    per_chip = CH // rows_dev
    chips = n // per_chip
    img = lax.axis_index(axis)
    my_chip = img // per_chip
    me = img

    def dev_rows(p):
        return pl.ds(pl.multiple_of(p * rows_dev, rows_dev), rows_dev)

    def in_copy(p):
        return pltpu.make_async_remote_copy(src_ref=x_hbm.at[p], dst_ref=x_scr.at[dev_rows(me)], send_sem=in_send.at[p], recv_sem=in_recv.at[me],
                                            device_id={axis: p}, device_id_type=pl.DeviceIdType.MESH)

    def out_copy(p):
        return pltpu.make_async_remote_copy(src_ref=x_scr.at[dev_rows(p)], dst_ref=out_hbm.at[me], send_sem=out_send.at[p], recv_sem=out_recv.at[me],
                                            device_id={axis: p}, device_id_type=pl.DeviceIdType.MESH)

    def ring(k):
        return lax.rem(my_chip + k, chips)

    def in_chip(c):
        return ring(lax.rem(c + c // 2 + 2 * (c // 3), chips))

    def out_chip(c):
        return ring(lax.rem(10 - c + 3 * (c // 2) + 2 * (c // 3), chips))

    barrier = pltpu.get_barrier_semaphore()
    for k in range(1, n):
        pl.semaphore_signal(barrier, inc=1, device_id={axis: lax.rem(me + k, n)}, device_id_type=pl.DeviceIdType.MESH)
    hbm = dict(zip(WEIGHTS, (wq_hbm, wkv_hbm, wo_hbm, cwq_hbm, cwo_hbm, w1_hbm, w2_hbm)))
    cap_scr, c_scr = h_scr.at[:ncap, 2 * d:3 * d], h_scr.at[:, :d]
    wq, wkv = wqkv.at[:, :d], wqkv.at[:, d:]
    buf = dict(zip(WEIGHTS, (wq, wkv, wo, cwq, cwo, w1, w2)))

    def wcopies(name, layer):
        i = WEIGHTS.index(name)
        rows = buf[name].shape[0] // SLABS
        return [pltpu.make_async_copy(hbm[name].at[layer, pl.ds(s * rows, rows)], buf[name].at[pl.ds(s * rows, rows)], wsem.at[i, s]) for s in range(SLABS)]

    def wstart(name, layer):
        for c in wcopies(name, layer):
            c.start()

    def wwait(name, layer):
        for c in wcopies(name, layer):
            c.wait()

    capcopy = pltpu.make_async_copy(cap_hbm.at[img], cap_scr.at[pl.ds(0, cap_hbm.shape[1])], capsem)
    ccopies = [pltpu.make_async_copy(cwkv_hbm.at[l], w1.at[:, pl.ds(l * 2 * d, 2 * d)], csem.at[l]) for l in range(2)]
    own_in = pltpu.make_async_copy(x_hbm.at[me], x_scr.at[dev_rows(me)], own_sem.at[0])
    own_out = pltpu.make_async_copy(x_scr.at[dev_rows(me)], out_hbm.at[me], own_sem.at[1])
    own_in.start()
    partner = me + 1 - 2 * lax.rem(me, per_chip)
    cap_scr[cap_hbm.shape[1]:, :] = jnp.zeros((ncap - cap_hbm.shape[1], d), BF16)
    capcopy.start()
    for c in ccopies:
        c.start()
    pl.semaphore_wait(barrier, n - 1)
    in_copy(partner).start()
    for k in (1, 3, 2):
        for j in range(per_chip):
            in_copy(ring(k) * per_chip + j).start()
    for name in ('wq', 'wkv', 'wo', 'cwq', 'cwo', 'w2'):
        wstart(name, 0)

    pick = lax.broadcasted_iota(jnp.int32, (te_ref.shape[0], 1), 0) == img
    te = jnp.sum(jnp.where(pick, te_ref[...].astype(F32), 0.0), axis=0, keepdims=True)
    for l in range(2):
        for j in range(6):
            mods[l, j:j + 1, :] = te[:, j * d:(j + 1) * d] + tab_ref[j, l:l + 1, :].astype(F32)
    vb_scr[...] = jnp.full(vb_scr.shape, -jnp.inf, F32)
    valid = jnp.sum(jnp.where(pick, valid_ref[...], 0), axis=0, keepdims=True)
    vb = jnp.where(valid > 0, 0.0, -1e9 / HEAD_DIM ** -0.5).astype(F32)
    vb_scr[:, :valid.shape[1]] = jnp.broadcast_to(vb, (8, valid.shape[1]))
    bias_scr[...] = vb_scr[...].T[:, 0:1]

    def store_heads(ref, rows, val):
        for h in range(heads):
            ref[h, rows, :] = val[:, h * HEAD_DIM:(h + 1) * HEAD_DIM]

    def store_heads_t(ref, cols, val):
        vt = val.T
        for h in range(heads):
            ref[h, :, cols] = vt[h * HEAD_DIM:(h + 1) * HEAD_DIM, :].astype(BF16)

    def row(ref, layer):
        return ref[layer:layer + 1, :].astype(F32)

    def modulate(v, layer, j):
        return (norm(v) * (1.0 + mods[layer, j + 1:j + 2, :]) + mods[layer, j:j + 1, :]).astype(BF16)

    capcopy.wait()
    for l in range(2):
        ccopies[l].wait()
        for part in range(2):
            lo = l * 2 * d + part * d
            y = dotf(cap_scr[...], w1[:, lo:lo + d]) + cbkv_ref[l:l + 1, part * d:(part + 1) * d].astype(F32)
            if part == 0:
                store_heads(kc_scr.at[l], slice(None), y.astype(BF16))
            else:
                store_heads_t(vc_scr.at[l], slice(None), y)
    wstart('w1', 0)

    wwait('wq', 0)

    def wait_in(p):
        pltpu.make_async_remote_copy(src_ref=x_hbm.at[p], dst_ref=x_scr.at[dev_rows(p)], send_sem=in_send.at[p], recv_sem=in_recv.at[p],
                                     device_id={axis: p}, device_id_type=pl.DeviceIdType.MESH).wait_recv()

    def prep0(step, _):
        c = in_chip(step)

        @pl.when(step == 0)
        def _():
            own_in.wait()
            wait_in(partner)

        @pl.when(step > 0)
        def _():
            for j in range(per_chip):
                wait_in(c * per_chip + j)

        rows = pl.ds(pl.multiple_of(c * CH, CH), CH)
        u = modulate(x_scr[rows, :].astype(F32), 0, 0)
        store_heads(q_scr, rows, (dotf(u, wq[...]) + row(bq_ref, 0)).astype(BF16))
        uf = u.astype(F32)
        parts = []
        for r in range(CH // width // 2):
            cols = []
            for j in range(d // 128):
                u_scr[j] = uf[2 * r * width:2 * (r + 1) * width, j * 128:(j + 1) * 128]
                acc = None
                for a in range(2):
                    for b in range(2):
                        w = cw_ref[a, b:b + 1, j * 128:(j + 1) * 128].astype(F32)
                        v = u_scr[j, pl.ds(a * width + b, width // 2, stride=2), :] * w
                        acc = v if acc is None else acc + v
                cols.append(acc)
            parts.append(jnp.concatenate(cols, axis=1))
        e = jnp.concatenate(parts, axis=0) + cb_ref[...].reshape(1, d).astype(F32)
        y = norm(e) * g_ref[...].reshape(1, d).astype(F32) + gb_ref[...].reshape(1, d).astype(F32)
        c_scr[pl.ds(pl.multiple_of(c * (CH // 4), CH // 4), CH // 4), :] = y.astype(BF16)
        return 0

    lax.fori_loop(0, t // CH, prep0, 0)
    wstart('wq', 1)
    in_copy(partner).wait_send()
    for k in (1, 3, 2):
        for j in range(per_chip):
            in_copy(ring(k) * per_chip + j).wait_send()
    wwait('wkv', 0)
    y = dotf(c_scr[...], wkv[...]) + row(bkv_ref, 0)
    store_heads(k_scr, slice(0, nkeys0), y[:, :d].astype(BF16))
    store_heads_t(vt_scr, slice(0, nkeys0), y[:, d:])
    wstart('wkv', 1)

    def tail(layer, tq, nkeys, sx, sy, unroll, cg):
        for name in ('wo', 'cwq', 'cwo', 'w1', 'w2'):
            wwait(name, layer)
        last = t // tq - 1
        kb = min(nkeys, 256)
        halves = tq // CH

        def chunk(c, _):
            base = pl.multiple_of((c if layer == 0 else out_chip(c)) * tq, tq)
            rows = pl.ds(base, tq)
            half = [pl.ds(pl.multiple_of(base + i * CH, CH), CH) for i in range(halves)]

            if layer == 0:
                def self_half(i, _):
                    r = pl.ds(pl.multiple_of(base + i * CH, CH), CH)
                    attention(lambda h: q_scr[h, r, :], lambda h, j: k_scr[h, j * kb:(j + 1) * kb, :], lambda h, j: vt_scr[h, :, j * kb:(j + 1) * kb],
                              ot.at[:, :, pl.ds(pl.multiple_of(i * CH, CH), CH)], sa, sb, nkeys // kb, kb, heads, None, 1, 4)
                    return 0

                lax.fori_loop(0, halves, self_half, 0)
            else:
                attention(lambda h: q_scr[h, rows, :], lambda h, i: k_scr[h, i * kb:(i + 1) * kb, :], lambda h, i: vt_scr[h, :, i * kb:(i + 1) * kb],
                          ot.at[:, :, :tq], sx, sy, nkeys // kb, kb, heads, None, unroll)
            for i in range(halves):
                o = ot[:, :, i * CH:(i + 1) * CH].reshape(d, CH).T.astype(BF16)
                x = x_scr[half[i], :].astype(F32)
                x = (x + mods[layer, 2:3, :] * (dotf(o, wo[...]) + row(bo_ref, layer))).astype(BF16)
                x_scr[half[i], :] = x
                store_heads(q_scr, half[i], (dotf(x, cwq[...]) + row(cbq_ref, layer)).astype(BF16))
            attention(lambda h: q_scr[h, rows, :], lambda h, i: kc_scr[layer, h], lambda h, i: vc_scr[layer, h],
                      ot.at[:, :, :tq], sx, sy, 1, ncap, heads, lambda i: bias_scr[...], heads // cg // 2, cg)
            for i in range(halves):
                o = ot[:, :, i * CH:(i + 1) * CH].reshape(d, CH).T.astype(BF16)
                x_scr[half[i], :] = (x_scr[half[i], :].astype(F32) + (dotf(o, cwo[...]) + row(cbo_ref, layer))).astype(BF16)

            def mlp(i, _):
                r = pl.ds(pl.multiple_of(base + i * CH, CH), CH)
                u = modulate(x_scr[r, :].astype(F32), layer, 3)
                fb = 512
                for j in range(f // fb):
                    sl = slice(j * fb, (j + 1) * fb)
                    h_scr[:, sl] = gelu(dotf(u, w1[:, sl]) + b1_ref[layer:layer + 1, sl].astype(F32)).astype(BF16)
                y = dotf(h_scr[...], w2[...]) + row(b2_ref, layer)
                x_scr[r, :] = (x_scr[r, :].astype(F32) + mods[layer, 5:6, :] * y).astype(BF16)
                return 0

            if halves == 1:
                mlp(0, 0)
            else:
                lax.fori_loop(0, halves, mlp, 0)
            if layer == 1:
                @pl.when(c < last)
                def _():
                    for j in range(per_chip):
                        out_copy(out_chip(c) * per_chip + j).start()

                @pl.when(c == last)
                def _():
                    out_copy(partner).start()
                    own_out.start()
            return 0

        lax.fori_loop(0, t // tq, chunk, 0)

    tail(0, 2 * CH, nkeys0, sc, sd, 4, 2)
    for name in ('wo', 'cwq', 'cwo', 'w1', 'w2'):
        wstart(name, 1)

    wwait('wq', 1)
    wwait('wkv', 1)

    def prep1(c, _):
        rows = pl.ds(pl.multiple_of(c * CH, CH), CH)
        u = modulate(x_scr[rows, :].astype(F32), 1, 0)
        y = dotf(u, wqkv[...])
        store_heads(q_scr, rows, (y[:, :d] + row(bq_ref, 1)).astype(BF16))
        store_heads(k_scr, rows, (y[:, d:2 * d] + bkv_ref[1:2, :d].astype(F32)).astype(BF16))
        store_heads_t(vt_scr, rows, y[:, 2 * d:] + bkv_ref[1:2, d:].astype(F32))
        return 0

    lax.fori_loop(0, t // CH, prep1, 0)
    tail(1, CH, t, sa, sb, 8, 4)

    def wait_out(p):
        pltpu.make_async_remote_copy(src_ref=x_scr.at[dev_rows(p)], dst_ref=out_hbm.at[p], send_sem=out_send.at[p], recv_sem=out_recv.at[p],
                                     device_id={axis: p}, device_id_type=pl.DeviceIdType.MESH).wait_recv()

    own_out.wait()
    for k in range(1, n):
        p = lax.rem(me + k, n)
        out_copy(p).wait_send()
        wait_out(p)


def image_core(x, caption, cap_valid, time_emb, axis, width, ada_table, attn_wq, attn_bq, attn_wkv, attn_bkv, attn_wo, attn_bo, comp_w, comp_b, cnorm_g, cnorm_b, cross_wq, cross_bq, cross_wkv, cross_bkv, cross_wo, cross_bo, mlp_w1, mlp_b1, mlp_w2, mlp_b2):
    n, rows_dev, d = x.shape
    t = n * rows_dev
    f = mlp_w1.shape[2]
    heads = d // HEAD_DIM
    ncap = -(-caption.shape[1] // 128) * 128
    vmem = [cap_valid, time_emb, jnp.swapaxes(ada_table, 0, 1), attn_bq, attn_bkv, attn_bo, comp_w, comp_b, cnorm_g, cnorm_b, cross_bq, cross_bkv, cross_bo, mlp_b1, mlp_b2]
    weights = [attn_wq, attn_wkv, attn_wo, cross_wq, cross_wkv, cross_wo, mlp_w1, mlp_w2]
    anyspec = pl.BlockSpec(memory_space=pl.ANY)
    V = pltpu.VMEM
    scratch = [V((d, 3 * d), BF16), V((d, d), BF16), V((d, d), BF16), V((d, d), BF16), V((d, f), BF16), V((f, d), BF16),
               V((t, d), BF16), V((heads, t, HEAD_DIM), BF16), V((heads, t, HEAD_DIM), BF16), V((heads, HEAD_DIM, t), BF16),
               V((2, heads, ncap, HEAD_DIM), BF16), V((2, heads, HEAD_DIM, ncap), BF16), V((8, ncap), F32), V((ncap, 1), F32), V((2, 6, d), F32),
               V((t, CH), F32), V((t, CH), F32), V((t // 4, 2 * CH), F32), V((t // 4, 2 * CH), F32), V((heads, HEAD_DIM, 2 * CH), F32), V((CH, f), BF16),
               V((d // 128, 2 * width, 128), F32),
               pltpu.SemaphoreType.DMA((len(WEIGHTS), SLABS)), pltpu.SemaphoreType.DMA((2,)), pltpu.SemaphoreType.DMA] + [pltpu.SemaphoreType.DMA((n,))] * 4 + [pltpu.SemaphoreType.DMA((2,))]
    return pl.pallas_call(
        functools.partial(mega_kernel, axis=axis, width=width),
        in_specs=[anyspec, anyspec] + [pl.BlockSpec(memory_space=V)] * len(vmem) + [anyspec] * len(weights),
        out_specs=pl.BlockSpec(memory_space=V), out_shape=V(x.shape, BF16), scratch_shapes=scratch,
        compiler_params=pltpu.CompilerParams(collective_id=0, has_side_effects=True, vmem_limit_bytes=VLIM),
        name="blocks",
    )(x, caption, *vmem, *weights)


def solution(mesh):
    in_specs = (P('dp', 'sp', None, None), P('dp', None, None), P('dp', None), P('dp', None)) + (P(),) * 21
    out_specs = P('dp', 'sp', None, None)
    n = mesh.shape['sp']

    def device_fn(tokens, caption, cap_valid, time_emb, *weights):
        b, rows, width, d = tokens.shape
        assert b == n and n * rows * width == 4 * CH and CH % (rows * width) == 0
        return image_core(tokens.reshape(b, rows * width, d), caption, cap_valid, time_emb, 'sp', width, *weights).reshape(tokens.shape)

    return jax.shard_map(device_fn, mesh=mesh, in_specs=in_specs, out_specs=out_specs, check_vma=False)
```
